128 devices in a mesh: dp: 32 (over z, y, core), mp: 4 (over x).
Axes of the slice: x: 4, y: 4, z: 4, core: 2. Of those that a mesh axis runs over, the one named last changes fastest.
Arguments:
- ids: int32 [32768], P('dp'), may hold values from 0 to 16777215, as said below
- hash_a: int32 [1024], replicated, may hold values from 1 to 16383
- hash_b: int32 [1024], replicated, may hold values from 0 to 16383
- hash_p: int32 [1024], replicated, may hold values from 16384 to 32767
- hash_m: int32 [1024], replicated, may hold values from 4096 to 16383
- w_in: bfloat16 [1024, 2048], P(None, 'mp'), may hold values from -0.1875 to 0.1875
- w_mid: bfloat16 [2, 2048, 2048], P(None, None, 'mp'), may hold values from -0.125 to 0.125
- w_out: bfloat16 [2048, 64], P('mp'), may hold values from -0.125 to 0.125
- bn_gain: float32 [3, 2048], P(None, 'mp'), may hold values from 0.25 to 1.75
- bn_bias: float32 [3, 2048], P(None, 'mp'), may hold values from -3 to 3
- target: float32 [32768, 64], P('dp'), may hold values from -6 to 6
Outputs:
- grad_w_in: float32 [1024, 2048], P('dp', 'mp')
- grad_w_mid: float32 [2, 2048, 2048], P(None, 'dp', 'mp')
- grad_w_out: float32 [2048, 64], P(('mp', 'dp'))
- grad_gain: float32 [3, 2048], P(None, 'mp')
- grad_bias: float32 [3, 2048], P(None, 'mp')
The draws below stay inside these ranges and needn't reach their ends.
Inputs may be any that keep to these rules, and one draw needn't show every extreme that they name: The number of distinct ids among one device's 1024 rows differs from device to device, from one to many.
All inputs are finite; a program needn't handle non-finite values.
Results may differ from the reference program's by a relative error of at most 0.02.
Values may be sent and summed in bfloat16 or wider, within the bound.
No kernel may reach another device: no remote copies, remote signals or barrier semaphores. Data moves between devices by JAX's collectives and lax.ppermute only.
A program may use at most 128 MiB of HBM per device.

```python
import math
import jax
import jax.numpy as jnp
from jax import lax

K = 1024
HID = 2048
OUT = 64
LAYERS = 3
ROWS_DEV = 1024
BATCH = 32768


def draw_ids(key, part):
    level_key = jax.random.fold_in(key, 11)
    pool_key = jax.random.fold_in(key, 12)
    pick_key = jax.random.fold_in(key, 13)
    blocks = BATCH // ROWS_DEV
    levels = jax.random.randint(level_key, (blocks,), 0, 10)
    distinct = jnp.left_shift(jnp.ones((blocks,), jnp.int32), levels)
    pool = jax.random.randint(pool_key, (blocks, 1024), 0, 16777216)
    picks = jax.random.randint(pick_key, (blocks, ROWS_DEV), 0, 1073741824) % distinct[:, None]
    return jnp.take_along_axis(pool, picks, axis=1).reshape(-1).astype(jnp.int32)


def set_ends(result, rng, smallest, high):
    shape = result.shape
    index_at = [jax.random.randint(jax.random.fold_in(rng, axis), (), 0, shape[axis]) for axis in range(len(shape))]
    result = result.at[tuple(index_at)].set(smallest)
    longest = shape.index(max(shape))
    index_at[longest] = (index_at[longest] + 1) % shape[longest]
    return result.at[tuple(index_at)].set(high)


def shard_levels(rng, shape, pieces, least, high):
    factor_of = 1.0
    for position, blocks in pieces:
        heights = jax.random.uniform(jax.random.fold_in(jax.random.fold_in(rng, 6), position), (blocks,), jnp.float32, least / len(pieces), high / len(pieces))
        factor_of = factor_of * jnp.repeat(jnp.exp(heights), shape[position] // blocks).reshape((-1,) + (1,) * (len(shape) - 1 - position))
    return factor_of


def gaussian(rng, dims, width, bound, split=(), dtype=jnp.bfloat16):
    factor_of = shard_levels(rng, dims, split, -0.22, 0.18) if split else 1.0
    array = jax.random.normal(rng, dims, jnp.float32) * width * factor_of
    return jnp.minimum(jnp.maximum(array, -bound), bound).astype(dtype)


def setup_inputs(seed: int = 0) -> dict:
    splits = jax.random.split(jax.random.key(seed), 12)
    ids = draw_ids(jax.random.fold_in(splits[11], 71), 0)
    hash_a = set_ends(jax.random.randint(splits[1], (K,), 1, 16384), jax.random.fold_in(splits[1], 1), 1, 16383).astype(jnp.int32)
    hash_b = set_ends(jax.random.randint(splits[2], (K,), 0, 16384), jax.random.fold_in(splits[2], 1), 0, 16383).astype(jnp.int32)
    hash_p = set_ends(jax.random.randint(splits[3], (K,), 16384, 32768), jax.random.fold_in(splits[3], 1), 16384, 32767).astype(jnp.int32)
    hash_m = set_ends(jax.random.randint(splits[4], (K,), 4096, 16384), jax.random.fold_in(splits[4], 1), 4096, 16383).astype(jnp.int32)
    w_in = gaussian(splits[5], (K, HID), K ** -0.5, 0.1875, ((1, 4),))
    w_mid = gaussian(splits[6], (LAYERS - 1, HID, HID), HID ** -0.5, 0.125, ((2, 4),))
    w_out = gaussian(splits[7], (HID, OUT), HID ** -0.5, 0.125, ((0, 4),))
    bn_gain = jnp.clip(1.0 + 0.15 * jax.random.normal(splits[8], (LAYERS, HID), jnp.float32), 0.25, 1.75)
    bn_bias = gaussian(splits[9], (LAYERS, HID), 0.5, 3.0, ((1, 4),), jnp.float32)
    target = gaussian(splits[10], (BATCH, OUT), 1.0, 6.0, ((0, 32),), jnp.float32)
    return {"ids": ids, "hash_a": hash_a, "hash_b": hash_b, "hash_p": hash_p, "hash_m": hash_m, "w_in": w_in, "w_mid": w_mid, "w_out": w_out, "bn_gain": bn_gain, "bn_bias": bn_bias, "target": target}


epsilon_norm = 1e-05

def encode(ids, hash_a, hash_b, hash_p, hash_m):
    reduced = ids[:, None] % hash_p[None, :]
    hashed = (hash_a[None, :] * reduced + hash_b[None, :]) % hash_p[None, :] % hash_m[None, :]
    scaled = 2.0 * hashed.astype(jnp.float32) / (hash_m[None, :] - 1).astype(jnp.float32) - 1.0
    return scaled.astype(jnp.bfloat16)

def mish_act(values):
    return values * jnp.tanh(jax.nn.softplus(values))

def mish_slope(values):
    tangent = jnp.tanh(jax.nn.softplus(values))
    return tangent + values * (1.0 - tangent * tangent) * jax.nn.sigmoid(values)

def reference(ids, hash_a, hash_b, hash_p, hash_m, w_in, w_mid, w_out, bn_gain, bn_bias, target):
    inputs = [encode(ids, hash_a, hash_b, hash_p, hash_m)]
    saved = []
    for layer_at in range(LAYERS):
        weights = w_in if layer_at == 0 else w_mid[layer_at - 1]
        summed = jnp.dot(inputs[-1], weights, preferred_element_type=jnp.float32)
        average = lax.optimization_barrier(jnp.mean(summed, axis=0))
        centered = summed - average
        spread = lax.optimization_barrier(jnp.mean(centered * centered, axis=0))
        inverse = 1.0 / jnp.sqrt(spread + epsilon_norm)
        normed = centered * inverse
        shifted = bn_gain[layer_at] * normed + bn_bias[layer_at]
        inputs.append(mish_act(shifted).astype(jnp.bfloat16))
        saved.append((normed, inverse, shifted))
    predicted = jnp.dot(inputs[-1], w_out, preferred_element_type=jnp.float32)
    residual_out = ((predicted - target) / math.sqrt(BATCH)).astype(jnp.bfloat16)
    grad_out = jnp.dot(inputs[-1].T, residual_out, preferred_element_type=jnp.float32)
    upstream = jnp.dot(residual_out, w_out.T, preferred_element_type=jnp.float32)
    grads_gain = []
    grads_bias = []
    grads_weight = []
    for layer_at in reversed(range(LAYERS)):
        normed, inverse, shifted = saved[layer_at]
        slope_a = upstream * mish_slope(shifted)
        bias_sum = lax.optimization_barrier(jnp.sum(slope_a, axis=0))
        gain_sum = lax.optimization_barrier(jnp.sum(slope_a * normed, axis=0))
        slope_z = (bn_gain[layer_at] * inverse * (slope_a - bias_sum / BATCH - normed * gain_sum / BATCH)).astype(jnp.bfloat16)
        grads_weight.append(jnp.dot(inputs[layer_at].T, slope_z, preferred_element_type=jnp.float32))
        if layer_at > 0:
            upstream = jnp.dot(slope_z, w_mid[layer_at - 1].T, preferred_element_type=jnp.float32)
        grads_gain.append(gain_sum)
        grads_bias.append(bias_sum)
    grads_weight = grads_weight[::-1]
    grad_gain = jnp.stack(grads_gain[::-1])
    grad_bias = jnp.stack(grads_bias[::-1])
    return (grads_weight[0], jnp.stack(grads_weight[1:]), grad_out, grad_gain, grad_bias)
```

```python
import math

import jax
import jax.numpy as jnp
from jax import lax
from jax.sharding import PartitionSpec as P

epsilon_norm = 1e-05


def from_everyone(array, axis):
    size = lax.axis_size(axis)
    return lax.all_to_all(
        jnp.broadcast_to(array[None], (size, *array.shape)), axis, 0, 0, tiled=True
    )


def over_copies(array, axis):
    everything = from_everyone(array, axis)
    return jnp.sum(everything, axis=0)


def together(arrays, axis):
    ends = [0]
    for a in arrays:
        ends.append(ends[-1] + a.size)
    total = over_copies(jnp.concatenate([a.ravel() for a in arrays]), axis)
    return tuple((total[b:e].reshape(a.shape) for a, b, e in zip(arrays, ends, ends[1:])))


def of_everyone(array, axis):
    everything = from_everyone(array, axis)
    return jnp.sum(everything.astype(jnp.float32), axis=0)


def cut_along(array, dim, size):
    dims = array.shape
    parts = array.reshape(*dims[:dim], size, dims[dim] // size, *dims[dim + 1 :])
    return jnp.moveaxis(parts, dim, 0)


def sum_at_owner(array, axis, dim):
    size = lax.axis_size(axis)
    parts = lax.all_to_all(cut_along(array, dim, size), axis, 0, 0, tiled=True)
    return jnp.sum(parts.astype(jnp.float32), axis=0)


def float_mod(values, inverse, modulus):
    rest = values - jnp.floor(values * inverse) * modulus
    return jnp.where(rest >= modulus, rest - modulus, rest)


def encode(ids, hash_a, hash_b, hash_p, hash_m):
    modulus = hash_p.astype(jnp.float32)[None, :]
    buckets = hash_m.astype(jnp.float32)[None, :]
    below = 1.0 - 2.0**-21
    inverse_p = below / modulus
    inverse_m = below / buckets
    high = (hash_a // 128).astype(jnp.float32)[None, :]
    low = (hash_a % 128).astype(jnp.float32)[None, :]
    shift = hash_b.astype(jnp.float32)[None, :]
    step = 2.0 / (buckets - 1.0)
    reduced = float_mod(ids.astype(jnp.float32)[:, None], inverse_p, modulus)
    carried = float_mod(high * reduced, inverse_p, modulus)
    mixed = float_mod(carried * 128.0 + low * reduced + shift, inverse_p, modulus)
    hashed = float_mod(mixed, inverse_m, buckets)
    return lax.optimization_barrier((hashed * step - 1.0).astype(jnp.bfloat16))


def mish_act(values):
    return values * jnp.tanh(jax.nn.softplus(values))


def mish_slope(values):
    tangent = jnp.tanh(jax.nn.softplus(values))
    return tangent + values * (1.0 - tangent * tangent) * jax.nn.sigmoid(values)


def column_stats(summed, batch_total):
    totals, squares = together((jnp.sum(summed, axis=0), jnp.sum(summed * summed, axis=0)), "dp")
    average = totals / batch_total
    spread = squares / batch_total - average * average
    centered = summed - average
    inverse = 1.0 / jnp.sqrt(spread + epsilon_norm)
    return (centered * inverse, inverse)


def column_products(left_rows, right_rows):
    return jnp.dot(left_rows.T, right_rows, preferred_element_type=jnp.float32)


def per_device(ids, hash_a, hash_b, hash_p, hash_m, w_in, w_mid, w_out, bn_gain, bn_bias, target):
    batch_devices = lax.axis_size("dp")
    batch_total = ids.shape[0] * batch_devices
    layer_count = bn_gain.shape[0]
    encoded = encode(ids, hash_a, hash_b, hash_p, hash_m)
    full_inputs = []
    saved = []
    current = encoded
    for layer_at in range(layer_count):
        if layer_at == 0:
            whole_input = encoded
            summed = jnp.dot(whole_input, w_in, preferred_element_type=jnp.float32)
        else:
            whole_input = lax.all_gather(current, "mp", axis=1, tiled=True)
            summed = jnp.dot(whole_input, w_mid[layer_at - 1], preferred_element_type=jnp.float32)
        full_inputs.append(whole_input)
        normed, inverse = column_stats(summed, batch_total)
        shifted = bn_gain[layer_at] * normed + bn_bias[layer_at]
        current = mish_act(shifted).astype(jnp.bfloat16)
        saved.append((normed, inverse, shifted))
    partial_out = jnp.dot(current, w_out, preferred_element_type=jnp.float32)
    predicted = of_everyone(partial_out.astype(jnp.bfloat16), "mp").astype(jnp.float32)
    residual_out = ((predicted - target) / math.sqrt(batch_total)).astype(jnp.bfloat16)
    grad_out = sum_at_owner(column_products(current, residual_out).astype(jnp.bfloat16), "dp", 0)
    upstream = jnp.dot(residual_out, w_out.T, preferred_element_type=jnp.float32)
    grads_gain = []
    grads_bias = []
    grads_mid = []
    grad_first = None
    for layer_at in reversed(range(layer_count)):
        normed, inverse, shifted = saved[layer_at]
        slope_a = upstream * mish_slope(shifted)
        bias_sum, gain_sum = together(
            (jnp.sum(slope_a, axis=0), jnp.sum(slope_a * normed, axis=0)), "dp"
        )
        slope_z = (
            bn_gain[layer_at]
            * inverse
            * (slope_a - bias_sum / batch_total - normed * gain_sum / batch_total)
        ).astype(jnp.bfloat16)
        whole_input = full_inputs[layer_at]
        if layer_at == 0:
            grad_first = sum_at_owner(
                column_products(whole_input, slope_z).astype(jnp.bfloat16), "dp", 0
            )
        else:
            grads_mid.append(
                lax.psum_scatter(
                    column_products(whole_input, slope_z).astype(jnp.bfloat16),
                    "dp",
                    scatter_dimension=0,
                    tiled=True,
                ).astype(jnp.float32)
            )
            weights = w_mid[layer_at - 1]
            partial_in = jnp.dot(slope_z, weights.T, preferred_element_type=jnp.float32)
            upstream = lax.psum_scatter(
                partial_in.astype(jnp.bfloat16), "mp", scatter_dimension=1, tiled=True
            ).astype(jnp.float32)
        grads_gain.append(gain_sum)
        grads_bias.append(bias_sum)
    grad_mid = jnp.stack(grads_mid[::-1])
    grad_gain = jnp.stack(grads_gain[::-1])
    grad_bias = jnp.stack(grads_bias[::-1])
    return (grad_first, grad_mid, grad_out, grad_gain, grad_bias)


def solution(mesh):
    return jax.shard_map(
        per_device,
        mesh=mesh,
        in_specs=(
            P("dp"),
            P(),
            P(),
            P(),
            P(),
            P(None, "mp"),
            P(None, None, "mp"),
            P("mp", None),
            P(None, "mp"),
            P(None, "mp"),
            P("dp", None),
        ),
        out_specs=(
            P("dp", "mp"),
            P(None, "dp", "mp"),
            P(("mp", "dp"), None),
            P(None, "mp"),
            P(None, "mp"),
        ),
        check_vma=False,
    )
```

```python
import math

import jax
import jax.numpy as jnp
from jax import lax
from jax.sharding import Mesh, PartitionSpec as P

epsilon_norm = 1e-05
chips = ("z", "y", "x")
plane = ("z", "y")
rows_axes = ("z", "y", "c")
float32 = jnp.float32
bfloat16 = jnp.bfloat16


def swap_cores(array):
    return lax.ppermute(array, "c", [(0, 1), (1, 0)])


def from_everyone(array, axis):
    size = lax.axis_size(axis)
    return lax.all_to_all(
        jnp.broadcast_to(array[None], (size, *array.shape)), axis, 0, 0, tiled=True
    )


def total_of(pair, axis):
    rows = jnp.concatenate(pair)[None]
    total = jnp.sum(from_everyone(rows, axis), axis=(0, 1))
    return jnp.split(total, len(pair))


def float_mod(values, inverse, modulus):
    rest = values - jnp.floor(values * inverse) * modulus
    return jnp.where(rest >= modulus, rest - modulus, rest)


def encode(ids, hash_a, hash_b, hash_p, hash_m):
    modulus = hash_p.astype(float32)[None, :]
    buckets = hash_m.astype(float32)[None, :]
    below = 1.0 - 2.0**-21
    inverse_p = below / modulus
    inverse_m = below / buckets
    high = (hash_a // 128).astype(float32)[None, :]
    low = (hash_a % 128).astype(float32)[None, :]
    shift = hash_b.astype(float32)[None, :]
    step = 2.0 / (buckets - 1.0)
    reduced = float_mod(ids.astype(float32)[:, None], inverse_p, modulus)
    carried = float_mod(high * reduced, inverse_p, modulus)
    mixed = float_mod(carried * 128.0 + low * reduced + shift, inverse_p, modulus)
    hashed = float_mod(mixed, inverse_m, buckets)
    return lax.optimization_barrier((hashed * step - 1.0).astype(bfloat16))


def mish_act(values):
    power = jnp.exp(jnp.minimum(values, 30.0))
    ratio = power * (power + 2.0)
    return values * (ratio / (ratio + 2.0))


def mish_slope(values):
    power = jnp.exp(jnp.minimum(values, 30.0))
    ratio = power * (power + 2.0)
    inverse = 1.0 / (ratio + 2.0)
    return inverse * (ratio + 4.0 * values * (power * (power + 1.0)) * inverse)


def dot(left, right):
    return jnp.dot(left, right, preferred_element_type=float32)


def dot_rows(left, right):
    return lax.dot_general(left, right, (((0,), (0,)), ((), ())), preferred_element_type=float32)


def dot_back(left, right):
    return lax.dot_general(left, right, (((1,), (1,)), ((), ())), preferred_element_type=float32)


def normalise(summed, axis, batch_total):
    totals, squares = total_of((jnp.sum(summed, axis=0), jnp.sum(summed * summed, axis=0)), axis)
    average = totals / batch_total
    spread = squares / batch_total - average * average
    return average, 1.0 / jnp.sqrt(spread + epsilon_norm)


def flip_rows(array):
    half = array.shape[0] // 2
    return jnp.concatenate([array[half:], array[:half]])


def per_device(ids, hash_a, hash_b, hash_p, hash_m, w_in, w_mid, w_out, bn_gain, bn_bias, target):
    core = lax.axis_index("c")
    lane = lax.axis_index("x")
    first = core == 0
    mp = lax.axis_size("x")
    planes = lax.axis_size(plane)
    rows, batch_devices = ids.shape[0], lax.axis_size(rows_axes)
    batch_total = rows * batch_devices
    width = w_in.shape[1]
    half = width // 2
    own = mp * half
    hidden = mp * width
    part = rows // mp
    out = w_out.shape[1]

    def in_order(mine, other):
        return jnp.where(first, mine, other), jnp.where(first, other, mine)

    w2_part = lax.dynamic_slice_in_dim(w_mid[0], core * half, half, axis=1)
    w2 = lax.all_gather(w2_part, "x", axis=1, tiled=True)
    w3_part = lax.dynamic_slice_in_dim(w_mid[1], core * half, half, axis=1)
    w3_low, w3_high = jnp.split(w3_part.reshape(mp, 2, half, half), 2, axis=1)
    w3_part = jnp.concatenate(
        [jnp.where(first, w3_low, w3_high), jnp.where(first, w3_high, w3_low)]
    ).reshape(hidden, half)
    w3 = lax.all_gather(w3_part, "x", axis=1, tiled=True)
    w3_own, w3_other = w3[:own], w3[own:]

    def half_of(array, axis):
        return lax.dynamic_slice_in_dim(array, core * half, half, axis=axis)

    small = jnp.concatenate(
        [
            half_of(w_out, 0).astype(float32).ravel(),
            half_of(bn_gain[1:], 1).ravel(),
            half_of(bn_bias[1:], 1).ravel(),
        ]
    )
    small = from_everyone(small.reshape(1, -1, 128), "x").reshape(mp, -1)
    w_out_own = small[:, : half * out].reshape(own, out).astype(bfloat16)
    vectors = small[:, half * out :].reshape(mp, 4, half).transpose(1, 0, 2).reshape(4, own)
    gain2, gain3, bias2, bias3 = vectors
    target_own = lax.dynamic_slice_in_dim(target, lane * part, part, axis=0)
    wanted = jnp.concatenate([target_own, swap_cores(target_own)])

    encoded = encode(ids, hash_a, hash_b, hash_p, hash_m)
    z1 = dot(encoded, w_in)
    mean1, inv1 = normalise(z1, rows_axes, batch_total)
    n1 = (z1 - mean1) * inv1
    a1 = bn_gain[0] * n1 + bn_bias[0]
    x1 = mish_act(a1).astype(bfloat16)
    x1_own = lax.all_to_all(x1, "x", 0, 1, tiled=True)
    x1_all = jnp.concatenate([x1_own, swap_cores(x1_own)])
    z2 = dot(x1_all, w2)
    mean2, inv2 = normalise(z2, chips, batch_total)
    n2 = (z2 - mean2) * inv2
    a2 = gain2 * n2 + bias2
    x2 = mish_act(a2).astype(bfloat16)
    x2_other = swap_cores(flip_rows(x2))
    z3 = dot(x2, w3_own) + dot(x2_other, w3_other)
    mean3, inv3 = normalise(z3, chips, batch_total)
    n3 = (z3 - mean3) * inv3
    a3 = gain3 * n3 + bias3
    x3 = mish_act(a3).astype(bfloat16)

    y_part = dot(x3, w_out_own)
    predicted = y_part + swap_cores(flip_rows(y_part))
    g_y = ((predicted - wanted) / math.sqrt(batch_total)).astype(bfloat16)
    g_out = dot_rows(x3, g_y).reshape(mp, planes // 2, 2, -1, out)
    keep_out = jnp.where(first, g_out[:, :, 0], g_out[:, :, 1])
    send_out = jnp.where(first, g_out[:, :, 1], g_out[:, :, 0]).astype(bfloat16)
    keep_out = keep_out.astype(bfloat16)
    g_out = jnp.stack(in_order(keep_out, swap_cores(send_out)))
    g_out = g_out.transpose(0, 2, 1, 3, 4).reshape(planes * mp, 1, -1).astype(float32)

    def last_sums(array):
        parts = lax.all_to_all(
            array.reshape(planes, array.shape[0] // planes, -1), plane, 0, 0, tiled=True
        )
        return jnp.sum(parts.astype(float32), axis=0)

    u3 = dot_back(g_y, w_out_own)
    s3 = u3 * mish_slope(a3)
    bias_sum3, gain_sum3 = total_of((jnp.sum(s3, axis=0), jnp.sum(s3 * n3, axis=0)), chips)
    e3 = (gain3 * inv3 * (s3 - bias_sum3 / batch_total - n3 * gain_sum3 / batch_total)).astype(
        bfloat16
    )
    u2_send = dot_back(e3, w3_other).astype(bfloat16)
    u2 = dot_back(e3, w3_own) + swap_cores(flip_rows(u2_send)).astype(float32)
    dw3 = jnp.concatenate([dot_rows(x2, e3), dot_rows(x2_other, e3)]).astype(bfloat16)
    dw3 = lax.psum_scatter(dw3, "x", scatter_dimension=1, tiled=True)

    s2 = u2 * mish_slope(a2)
    sums2 = jnp.concatenate([jnp.sum(s2, axis=0), jnp.sum(s2 * n2, axis=0)])
    message = jnp.concatenate(
        [jnp.broadcast_to(sums2[None, None], (planes * mp, 1, sums2.shape[0])), g_out], axis=2
    )
    message = jnp.sum(lax.all_to_all(message, chips, 0, 0, tiled=True), axis=(0, 1))
    bias_sum2, gain_sum2 = message[:own], message[own : 2 * own]
    grad_out = message[2 * own :].reshape(-1, out)
    e2 = (gain2 * inv2 * (s2 - bias_sum2 / batch_total - n2 * gain_sum2 / batch_total)).astype(
        bfloat16
    )
    u1_send = dot_back(e2[part:], w2).astype(bfloat16)
    u1_own = (dot_back(e2[:part], w2) + swap_cores(u1_send).astype(float32)).astype(bfloat16)
    u1 = lax.all_to_all(u1_own, "x", 1, 0, tiled=True).astype(float32)
    dw2 = dot_rows(x1_all, e2).astype(bfloat16)
    dw2 = lax.psum_scatter(dw2, "x", scatter_dimension=1, tiled=True)

    s1 = u1 * mish_slope(a1)
    bias_sum1, gain_sum1 = total_of((jnp.sum(s1, axis=0), jnp.sum(s1 * n1, axis=0)), rows_axes)
    e1 = (
        bn_gain[0] * inv1 * (s1 - bias_sum1 / batch_total - n1 * gain_sum1 / batch_total)
    ).astype(bfloat16)
    dw1 = dot_rows(encoded, e1).reshape(planes, 2, -1, width)
    keep1 = jnp.where(first, dw1[:, 0], dw1[:, 1])
    send1 = jnp.where(first, dw1[:, 1], dw1[:, 0]).astype(bfloat16)
    dw1 = (keep1 + swap_cores(send1).astype(float32)).astype(bfloat16)
    dw1 = lax.all_to_all(dw1, plane, 0, 0, tiled=True)
    grad_first = jnp.sum(dw1.astype(float32), axis=0)

    dw3 = dw3.reshape(2, mp, half, half)
    dw3 = jnp.stack(in_order(dw3[0], dw3[1]), axis=1).reshape(hidden, half)

    def finish(array):
        total = last_sums(array).reshape(hidden // planes, half)
        low, high = jnp.split(total, 2)
        mine = jnp.where(first, low, high)
        other = swap_cores(jnp.where(first, high, low))
        return jnp.concatenate(in_order(mine, other), axis=1)

    grad_mid = jnp.stack([finish(dw2), finish(dw3)])

    sums = jnp.stack([gain_sum2, gain_sum3, bias_sum2, bias_sum3]).reshape(4, mp, half)
    mine = lax.dynamic_index_in_dim(sums, lane, axis=1, keepdims=False)
    later = jnp.concatenate(in_order(mine, swap_cores(mine)), axis=1)
    grad_gain = jnp.stack([gain_sum1, later[0], later[1]])
    grad_bias = jnp.stack([bias_sum1, later[2], later[3]])
    return (grad_first, grad_mid, grad_out, grad_gain, grad_bias)


def solution(mesh):
    grid = Mesh(mesh.devices.reshape(4, 4, 2, 4), ("z", "y", "c", "x"))
    return jax.shard_map(
        per_device,
        mesh=grid,
        in_specs=(
            P(rows_axes),
            P(),
            P(),
            P(),
            P(),
            P(None, "x"),
            P(None, None, "x"),
            P("x", None),
            P(None, "x"),
            P(None, "x"),
            P(rows_axes, None),
        ),
        out_specs=(
            P(rows_axes, "x"),
            P(None, rows_axes, "x"),
            P(("x", "z", "y", "c"), None),
            P(None, "x"),
            P(None, "x"),
        ),
        check_vma=False,
    )
```

```python
import math

import jax
import jax.numpy as jnp
from jax import lax
from jax.sharding import Mesh, PartitionSpec as P

epsilon_norm = 1e-05
plane = ("z", "y")
over_chips = (("z", "y", "x"),)
over_chips_x_last = (("z", "y"), "x")
over_chips_z_last = (("y", "x"), "z")
over_rows = ("c", ("z", "y"))
rows_axes = ("z", "y", "c")
float32 = jnp.float32
bfloat16 = jnp.bfloat16


def swap_cores(array):
    return lax.ppermute(array, "c", [(0, 1), (1, 0)])


def from_everyone(array, axis):
    size = lax.axis_size(axis)
    return lax.all_to_all(
        jnp.broadcast_to(array[None], (size, *array.shape)), axis, 0, 0, tiled=True
    )


def sum_over(rows, stages):
    for axis in stages:
        if axis == "c":
            rows = rows + swap_cores(rows)
        else:
            rows = jnp.sum(from_everyone(rows, axis), axis=0)
    return rows[0]


def total_of(pair, stages):
    return jnp.split(sum_over(jnp.concatenate(pair)[None], stages), len(pair))


def float_mod(values, inverse, modulus):
    rest = values - jnp.floor(values * inverse) * modulus
    return jnp.where(rest >= modulus, rest - modulus, rest)


def encode(ids, hash_a, hash_b, hash_p, hash_m):
    modulus = hash_p.astype(float32)[None, :]
    buckets = hash_m.astype(float32)[None, :]
    below = 1.0 - 2.0**-21
    inverse_p = below / modulus
    inverse_m = below / buckets
    high = (hash_a // 128).astype(float32)[None, :]
    low = (hash_a % 128).astype(float32)[None, :]
    shift = hash_b.astype(float32)[None, :]
    step = 2.0 / (buckets - 1.0)
    reduced = float_mod(ids.astype(float32)[:, None], inverse_p, modulus)
    carried = float_mod(high * reduced, inverse_p, modulus)
    mixed = float_mod(carried * 128.0 + low * reduced + shift, inverse_p, modulus)
    hashed = float_mod(mixed, inverse_m, buckets)
    return lax.optimization_barrier((hashed * step - 1.0).astype(bfloat16))


def mish_act(values):
    power = jnp.exp(jnp.minimum(values, 30.0))
    ratio = power * (power + 2.0)
    return values * (ratio / (ratio + 2.0))


def mish_slope(values):
    power = jnp.exp(jnp.minimum(values, 30.0))
    ratio = power * (power + 2.0)
    inverse = 1.0 / (ratio + 2.0)
    return inverse * (ratio + 4.0 * values * (power * (power + 1.0)) * inverse)


def dot(left, right):
    return jnp.dot(left, right, preferred_element_type=float32)


def dot_rows(left, right):
    return lax.dot_general(left, right, (((0,), (0,)), ((), ())), preferred_element_type=float32)


def dot_back(left, right):
    return lax.dot_general(left, right, (((1,), (1,)), ((), ())), preferred_element_type=float32)


def normalise(summed, axis, batch_total):
    totals, squares = total_of((jnp.sum(summed, axis=0), jnp.sum(summed * summed, axis=0)), axis)
    average = totals / batch_total
    spread = squares / batch_total - average * average
    return average, 1.0 / jnp.sqrt(spread + epsilon_norm)


def flip_rows(array):
    half = array.shape[0] // 2
    return jnp.concatenate([array[half:], array[:half]])


def per_device(ids, hash_a, hash_b, hash_p, hash_m, w_in, w_mid, w_out, bn_gain, bn_bias, target):
    core = lax.axis_index("c")
    lane = lax.axis_index("x")
    first = core == 0
    mp = lax.axis_size("x")
    planes = lax.axis_size(plane)
    rows, batch_devices = ids.shape[0], lax.axis_size(rows_axes)
    batch_total = rows * batch_devices
    width = w_in.shape[1]
    half = width // 2
    own = mp * half
    hidden = mp * width
    part = rows // mp
    out = w_out.shape[1]

    def in_order(mine, other):
        return jnp.where(first, mine, other), jnp.where(first, other, mine)

    def weight_part(layer):
        start = (layer, 0, core * half)
        return lax.dynamic_slice(w_mid, start, (1, hidden, half)).reshape(hidden, half)

    w2 = lax.all_gather(weight_part(0), "x", axis=1, tiled=True)
    w3_low, w3_high = jnp.split(weight_part(1).reshape(mp, 2, half, half), 2, axis=1)
    w3_part = jnp.concatenate(in_order(w3_low, w3_high), axis=1).reshape(hidden, half)
    w3 = lax.all_gather(w3_part, "x", axis=1, tiled=True)

    def half_of(array, axis):
        return lax.dynamic_slice_in_dim(array, core * half, half, axis=axis)

    vectors = jnp.concatenate([half_of(bn_gain[1:], 1), half_of(bn_bias[1:], 1)])
    high = lax.reduce_precision(vectors, 8, 7)
    middle = lax.reduce_precision(vectors - high, 8, 7)
    low = vectors - high - middle
    small = jnp.concatenate(
        [
            half_of(w_out, 0).reshape(-1, width),
            jnp.concatenate([high, middle, low]).astype(bfloat16).reshape(-1, width),
        ]
    )
    small = jnp.pad(small, ((0, -small.shape[0] % 16), (0, 0)))
    target_own = lax.dynamic_slice_in_dim(target, lane * part, part, axis=0)
    wanted = jnp.concatenate([target_own, swap_cores(target_own)])

    encoded = encode(ids, hash_a, hash_b, hash_p, hash_m)
    z1 = dot(encoded, w_in)
    mean1, inv1 = normalise(z1, over_rows, batch_total)
    n1 = (z1 - mean1) * inv1
    a1 = bn_gain[0] * n1 + bn_bias[0]
    x1 = mish_act(a1).astype(bfloat16)
    message = jnp.concatenate(
        [x1.reshape(mp, part, width), jnp.broadcast_to(small[None], (mp, *small.shape))], axis=1
    )
    message = lax.all_to_all(message, "x", 0, 0, tiled=True)
    x1_own = message[:, :part].transpose(1, 0, 2).reshape(part, hidden)
    x1_all = jnp.concatenate([x1_own, swap_cores(x1_own)])
    small = message[:, part:].reshape(mp, -1)
    w_out_own = small[:, : half * out].reshape(own, out)
    vectors = small[:, half * out : half * out + 12 * half].astype(float32)
    vectors = vectors.reshape(mp, 3, 4, half)
    vectors = vectors[:, 0] + vectors[:, 1] + vectors[:, 2]
    gain2, gain3, bias2, bias3 = vectors.transpose(1, 0, 2).reshape(4, own)
    z2 = dot(x1_all, w2)
    mean2, inv2 = normalise(z2, over_chips_x_last, batch_total)
    n2 = (z2 - mean2) * inv2
    a2 = gain2 * n2 + bias2
    x2 = mish_act(a2).astype(bfloat16)
    x2_other = swap_cores(flip_rows(x2))
    x2_all = jnp.stack([x2.reshape(-1, mp, half), x2_other.reshape(-1, mp, half)], axis=2)
    x2_all = x2_all.reshape(-1, hidden)
    z3 = dot(x2_all, w3)
    mean3, inv3 = normalise(z3, over_chips, batch_total)
    n3 = (z3 - mean3) * inv3
    a3 = gain3 * n3 + bias3
    x3 = mish_act(a3).astype(bfloat16)

    y_part = dot(x3, w_out_own)
    predicted = y_part + swap_cores(flip_rows(y_part))
    g_y = ((predicted - wanted) / math.sqrt(batch_total)).astype(bfloat16)
    g_out = dot_rows(x3, g_y).reshape(mp, planes // 2, 2, -1, out)
    keep_out = jnp.where(first, g_out[:, :, 0], g_out[:, :, 1])
    send_out = jnp.where(first, g_out[:, :, 1], g_out[:, :, 0]).astype(bfloat16)
    keep_out = keep_out.astype(bfloat16)
    g_out = jnp.stack(in_order(keep_out, swap_cores(send_out)))
    depth, height = lax.axis_size("z"), lax.axis_size("y")
    g_out = g_out.transpose(0, 2, 1, 3, 4).reshape(depth, height * mp, -1)
    g_out = g_out.transpose(1, 0, 2).reshape(height * mp, 1, -1).astype(float32)

    u3 = dot_back(g_y, w_out_own)
    s3 = u3 * mish_slope(a3)
    bias_sum3, gain_sum3 = total_of((jnp.sum(s3, axis=0), jnp.sum(s3 * n3, axis=0)), over_chips)
    e3 = (gain3 * inv3 * (s3 - bias_sum3 / batch_total - n3 * gain_sum3 / batch_total)).astype(
        bfloat16
    )
    u2_part = dot_back(e3, w3).reshape(-1, mp, 2, half)
    u2_send = u2_part[:, :, 1].reshape(-1, own).astype(bfloat16)
    u2 = u2_part[:, :, 0].reshape(-1, own) + swap_cores(flip_rows(u2_send)).astype(float32)
    dw3 = dot_rows(x2_all, e3).astype(bfloat16)
    dw3 = lax.psum_scatter(dw3, "z", scatter_dimension=0, tiled=True)
    dw3 = lax.psum_scatter(dw3, "x", scatter_dimension=1, tiled=True)

    s2 = u2 * mish_slope(a2)
    sums2 = jnp.concatenate([jnp.sum(s2, axis=0), jnp.sum(s2 * n2, axis=0)])
    count = sums2.shape[0]
    sums2 = jnp.broadcast_to(sums2[None, None], (height * mp, 1, count))
    sums2 = jnp.concatenate([sums2, g_out], axis=2)
    sums2 = jnp.sum(lax.all_to_all(sums2, ("y", "x"), 0, 0, tiled=True), axis=(0, 1))
    g_out = sums2[count:].reshape(depth, -1)
    sums2 = jnp.broadcast_to(sums2[None, :count], (depth, count))
    sums2 = jnp.concatenate([sums2, g_out], axis=1)[:, None]
    sums2 = jnp.sum(lax.all_to_all(sums2, "z", 0, 0, tiled=True), axis=(0, 1))
    bias_sum2, gain_sum2 = sums2[:own], sums2[own:count]
    grad_out = sums2[count:].reshape(-1, out)
    e2 = (gain2 * inv2 * (s2 - bias_sum2 / batch_total - n2 * gain_sum2 / batch_total)).astype(
        bfloat16
    )
    u1_send = dot_back(e2[part:], w2).astype(bfloat16)
    u1_own = (dot_back(e2[:part], w2) + swap_cores(u1_send).astype(float32)).astype(bfloat16)
    u1 = lax.all_to_all(u1_own, "x", 1, 0, tiled=True).astype(float32)
    dw2 = dot_rows(x1_all, e2).astype(bfloat16)
    dw2 = lax.psum_scatter(dw2, "z", scatter_dimension=0, tiled=True)
    dw2 = lax.psum_scatter(dw2, "x", scatter_dimension=1, tiled=True)

    s1 = u1 * mish_slope(a1)
    bias_sum1, gain_sum1 = total_of((jnp.sum(s1, axis=0), jnp.sum(s1 * n1, axis=0)), over_rows)
    e1 = (
        bn_gain[0] * inv1 * (s1 - bias_sum1 / batch_total - n1 * gain_sum1 / batch_total)
    ).astype(bfloat16)
    dw1 = dot_rows(encoded, e1).reshape(planes, 2, -1, width)
    keep1 = jnp.where(first, dw1[:, 0], dw1[:, 1])
    send1 = jnp.where(first, dw1[:, 1], dw1[:, 0]).astype(bfloat16)
    dw1 = (keep1 + swap_cores(send1).astype(float32)).astype(bfloat16)
    dw1 = lax.all_to_all(dw1, plane, 0, 0, tiled=True)
    grad_first = jnp.sum(dw1.astype(float32), axis=0)

    dw2, dw3, grad_first = lax.optimization_barrier((dw2, dw3, grad_first))
    dw3 = dw3.reshape(2, half, half)
    dw3 = jnp.stack(in_order(dw3[0], dw3[1]))
    last = jnp.stack([dw2.reshape(height, -1, half), dw3.reshape(height, -1, half)], axis=1)
    last = lax.all_to_all(last, "y", 0, 0, tiled=True)
    last = jnp.sum(last.astype(float32), axis=0)
    low, high = jnp.split(last, 2, axis=1)
    other = swap_cores(jnp.where(first, high, low))
    grad_mid = jnp.concatenate(in_order(jnp.where(first, low, high), other), axis=2)

    sums = jnp.stack([gain_sum2, gain_sum3, bias_sum2, bias_sum3]).reshape(4, mp, half)
    mine = lax.dynamic_index_in_dim(sums, lane, axis=1, keepdims=False)
    later = jnp.concatenate(in_order(mine, swap_cores(mine)), axis=1)
    grad_gain = jnp.stack([gain_sum1, later[0], later[1]])
    grad_bias = jnp.stack([bias_sum1, later[2], later[3]])
    return (grad_first, grad_mid, grad_out, grad_gain, grad_bias)


def solution(mesh):
    grid = Mesh(mesh.devices.reshape(4, 4, 2, 4), ("z", "y", "c", "x"))
    return jax.shard_map(
        per_device,
        mesh=grid,
        in_specs=(
            P(rows_axes),
            P(),
            P(),
            P(),
            P(),
            P(None, "x"),
            P(None, None, "x"),
            P("x", None),
            P(None, "x"),
            P(None, "x"),
            P(rows_axes, None),
        ),
        out_specs=(
            P(rows_axes, "x"),
            P(None, rows_axes, "x"),
            P(("x", "z", "y", "c"), None),
            P(None, "x"),
            P(None, "x"),
        ),
        check_vma=False,
    )
```

```python
import math

import jax
import jax.numpy as jnp
from jax import lax
from jax.sharding import Mesh, PartitionSpec as P

epsilon_norm = 1e-05
plane = ("z", "y")
over_chips = (("z", "y", "x"),)
over_chips_x_last = (("z", "y"), "x")
over_chips_z_last = (("y", "x"), "z")
over_rows = ("c", ("z", "y"))
rows_axes = ("z", "y", "c")
float32 = jnp.float32
bfloat16 = jnp.bfloat16


def swap_cores(array):
    return lax.ppermute(array, "c", [(0, 1), (1, 0)])


def from_everyone(array, axis):
    size = lax.axis_size(axis)
    return lax.all_to_all(
        jnp.broadcast_to(array[None], (size, *array.shape)), axis, 0, 0, tiled=True
    )


def sum_over(rows, stages):
    for axis in stages:
        if axis == "c":
            rows = rows + swap_cores(rows)
        else:
            rows = jnp.sum(from_everyone(rows, axis), axis=0)
    return rows[0]


def total_of(pair, stages):
    return jnp.split(sum_over(jnp.concatenate(pair)[None], stages), len(pair))


def float_mod(values, inverse, modulus):
    rest = values - jnp.floor(values * inverse) * modulus
    return jnp.where(rest >= modulus, rest - modulus, rest)


def encode(ids, hash_a, hash_b, hash_p, hash_m):
    modulus = hash_p.astype(float32)[None, :]
    buckets = hash_m.astype(float32)[None, :]
    below = 1.0 - 2.0**-21
    inverse_p = below / modulus
    inverse_m = below / buckets
    high = (hash_a // 128).astype(float32)[None, :]
    low = (hash_a % 128).astype(float32)[None, :]
    shift = hash_b.astype(float32)[None, :]
    step = 2.0 / (buckets - 1.0)
    reduced = float_mod(ids.astype(float32)[:, None], inverse_p, modulus)
    carried = float_mod(high * reduced, inverse_p, modulus)
    mixed = float_mod(carried * 128.0 + low * reduced + shift, inverse_p, modulus)
    hashed = float_mod(mixed, inverse_m, buckets)
    return lax.optimization_barrier((hashed * step - 1.0).astype(bfloat16))


def mish_act(values):
    power = jnp.exp(jnp.minimum(values, 30.0))
    ratio = power * (power + 2.0)
    return values * (ratio / (ratio + 2.0))


def mish_slope(values):
    power = jnp.exp(jnp.minimum(values, 30.0))
    ratio = power * (power + 2.0)
    inverse = 1.0 / (ratio + 2.0)
    return inverse * (ratio + 4.0 * values * (power * (power + 1.0)) * inverse)


def dot(left, right):
    return jnp.dot(left, right, preferred_element_type=float32)


def dot_rows(left, right):
    return lax.dot_general(left, right, (((0,), (0,)), ((), ())), preferred_element_type=float32)


def dot_back(left, right):
    return lax.dot_general(left, right, (((1,), (1,)), ((), ())), preferred_element_type=float32)


def normalise(summed, axis, batch_total):
    totals, squares = total_of((jnp.sum(summed, axis=0), jnp.sum(summed * summed, axis=0)), axis)
    average = totals / batch_total
    spread = squares / batch_total - average * average
    return average, 1.0 / jnp.sqrt(spread + epsilon_norm)


def flip_rows(array):
    half = array.shape[0] // 2
    return jnp.concatenate([array[half:], array[:half]])


def per_device(ids, hash_a, hash_b, hash_p, hash_m, w_in, w_mid, w_out, bn_gain, bn_bias, target):
    core = lax.axis_index("c")
    lane = lax.axis_index("x")
    first = core == 0
    mp = lax.axis_size("x")
    depth, height = lax.axis_size("z"), lax.axis_size("y")
    planes = depth * height
    rows, batch_devices = ids.shape[0], lax.axis_size(rows_axes)
    batch_total = rows * batch_devices
    width = w_in.shape[1]
    half = width // 2
    own = mp * half
    hidden = mp * width
    part = rows // mp
    out = w_out.shape[1]

    def in_order(mine, other):
        return jnp.where(first, mine, other), jnp.where(first, other, mine)

    def weight_part(layer, row, count):
        start = (layer, row, core * half)
        return lax.dynamic_slice(w_mid, start, (1, count, half)).reshape(count, half)

    w2_rows = hidden // depth
    w2 = from_everyone(weight_part(0, lax.axis_index("z") * w2_rows, w2_rows), "x")
    w2 = lax.all_gather(jnp.concatenate(list(w2), axis=1), "z", axis=0, tiled=True)
    w3_low, w3_high = jnp.split(weight_part(1, 0, hidden).reshape(mp, 2, half, half), 2, axis=1)
    w3_part = jnp.concatenate(in_order(w3_low, w3_high), axis=1).reshape(hidden, half)
    w3 = lax.all_gather(w3_part, "x", axis=1, tiled=True)

    def half_of(array, axis):
        return lax.dynamic_slice_in_dim(array, core * half, half, axis=axis)

    vectors = jnp.concatenate([half_of(bn_gain[1:], 1), half_of(bn_bias[1:], 1)])
    high = lax.reduce_precision(vectors, 8, 7)
    middle = lax.reduce_precision(vectors - high, 8, 7)
    low = vectors - high - middle
    small = jnp.concatenate(
        [
            half_of(w_out, 0).reshape(-1, width),
            jnp.concatenate([high, middle, low]).astype(bfloat16).reshape(-1, width),
        ]
    )
    small = jnp.pad(small, ((0, -small.shape[0] % 16), (0, 0)))
    target_own = lax.dynamic_slice_in_dim(target, lane * part, part, axis=0)
    wanted = jnp.concatenate([target_own, swap_cores(target_own)])

    encoded = encode(ids, hash_a, hash_b, hash_p, hash_m)
    z1 = dot(encoded, w_in)
    mean1, inv1 = normalise(z1, over_rows, batch_total)
    n1 = (z1 - mean1) * inv1
    a1 = bn_gain[0] * n1 + bn_bias[0]
    x1 = mish_act(a1).astype(bfloat16)
    message = jnp.concatenate(
        [x1.reshape(mp, part, width), jnp.broadcast_to(small[None], (mp, *small.shape))], axis=1
    )
    message = lax.all_to_all(message, "x", 0, 0, tiled=True)
    x1_own = jnp.concatenate(list(message[:, :part]), axis=1)
    x1_all = jnp.concatenate([x1_own, swap_cores(x1_own)])
    small = message[:, part:].reshape(mp, -1)
    w_out_own = small[:, : half * out].reshape(own, out)
    vectors = small[:, half * out : half * out + 12 * half].astype(float32)
    vectors = vectors.reshape(mp, 3, 4, half)
    vectors = vectors[:, 0] + vectors[:, 1] + vectors[:, 2]
    gain2, gain3, bias2, bias3 = vectors.transpose(1, 0, 2).reshape(4, own)
    z2 = dot(x1_all, w2)
    mean2, inv2 = normalise(z2, over_chips_x_last, batch_total)
    n2 = (z2 - mean2) * inv2
    a2 = gain2 * n2 + bias2
    x2 = mish_act(a2).astype(bfloat16)
    x2_other = swap_cores(flip_rows(x2))
    blocks = zip(jnp.split(x2, mp, axis=1), jnp.split(x2_other, mp, axis=1))
    x2_all = jnp.concatenate([block for pair in blocks for block in pair], axis=1)
    z3 = dot(x2_all, w3)
    mean3, inv3 = normalise(z3, over_chips, batch_total)
    n3 = (z3 - mean3) * inv3
    a3 = gain3 * n3 + bias3
    x3 = mish_act(a3).astype(bfloat16)

    y_part = dot(x3, w_out_own)
    predicted = y_part + swap_cores(flip_rows(y_part))
    g_y = ((predicted - wanted) / math.sqrt(batch_total)).astype(bfloat16)
    g_out = dot_rows(x3, g_y).reshape(mp, planes // 2, 2, -1, out)
    keep_out = jnp.where(first, g_out[:, :, 0], g_out[:, :, 1])
    send_out = jnp.where(first, g_out[:, :, 1], g_out[:, :, 0]).astype(bfloat16)
    keep_out = keep_out.astype(bfloat16)
    g_out = jnp.stack(in_order(keep_out, swap_cores(send_out)))
    g_out = g_out.transpose(0, 2, 1, 3, 4).reshape(depth, height * mp, -1)
    g_out = g_out.transpose(1, 0, 2).reshape(height * mp, 1, -1).astype(float32)

    u3 = dot_back(g_y, w_out_own)
    s3 = u3 * mish_slope(a3)
    bias_sum3, gain_sum3 = total_of((jnp.sum(s3, axis=0), jnp.sum(s3 * n3, axis=0)), over_chips)
    e3 = (gain3 * inv3 * (s3 - bias_sum3 / batch_total - n3 * gain_sum3 / batch_total)).astype(
        bfloat16
    )
    u2_part = jnp.split(dot_back(e3, w3), 2 * mp, axis=1)
    u2_send = jnp.concatenate(u2_part[1::2], axis=1).astype(bfloat16)
    u2 = jnp.concatenate(u2_part[::2], axis=1)
    u2 = u2 + swap_cores(flip_rows(u2_send)).astype(float32)
    dw3 = dot_rows(x2_all, e3).astype(bfloat16)
    dw3 = lax.psum_scatter(dw3, "z", scatter_dimension=0, tiled=True)
    dw3 = lax.psum_scatter(dw3, "x", scatter_dimension=1, tiled=True)

    s2 = u2 * mish_slope(a2)
    sums2 = jnp.concatenate([jnp.sum(s2, axis=0), jnp.sum(s2 * n2, axis=0)])
    count = sums2.shape[0]
    sums2 = jnp.broadcast_to(sums2[None, None], (height * mp, 1, count))
    sums2 = jnp.concatenate([sums2, g_out], axis=2)
    sums2 = jnp.sum(lax.all_to_all(sums2, ("y", "x"), 0, 0, tiled=True), axis=(0, 1))
    g_out = sums2[count:].reshape(depth, -1)
    sums2 = jnp.broadcast_to(sums2[None, :count], (depth, count))
    sums2 = jnp.concatenate([sums2, g_out], axis=1)[:, None]
    sums2 = jnp.sum(lax.all_to_all(sums2, "z", 0, 0, tiled=True), axis=(0, 1))
    bias_sum2, gain_sum2 = sums2[:own], sums2[own:count]
    grad_out = sums2[count:].reshape(-1, out)
    e2 = (gain2 * inv2 * (s2 - bias_sum2 / batch_total - n2 * gain_sum2 / batch_total)).astype(
        bfloat16
    )
    u1_send = dot_back(e2[part:], w2).astype(bfloat16)
    u1_own = (dot_back(e2[:part], w2) + swap_cores(u1_send).astype(float32)).astype(bfloat16)
    u1 = lax.all_to_all(u1_own, "x", 1, 0, tiled=True).astype(float32)
    dw2 = dot_rows(x1_all, e2).astype(bfloat16)
    dw2 = lax.psum_scatter(dw2, "z", scatter_dimension=0, tiled=True)
    dw2 = jnp.stack([b.reshape(height, -1, half) for b in jnp.split(dw2, mp, axis=1)], axis=1)
    dw2 = lax.all_to_all(dw2.reshape(height * mp, -1, half), ("y", "x"), 0, 0, tiled=True)
    dw2 = jnp.sum(dw2.astype(float32), axis=0)

    s1 = u1 * mish_slope(a1)
    bias_sum1, gain_sum1 = total_of((jnp.sum(s1, axis=0), jnp.sum(s1 * n1, axis=0)), over_rows)
    e1 = (
        bn_gain[0] * inv1 * (s1 - bias_sum1 / batch_total - n1 * gain_sum1 / batch_total)
    ).astype(bfloat16)
    dw1 = dot_rows(encoded, e1).reshape(planes, 2, -1, width)
    keep1 = jnp.where(first, dw1[:, 0], dw1[:, 1])
    send1 = jnp.where(first, dw1[:, 1], dw1[:, 0]).astype(bfloat16)
    dw1 = (keep1 + swap_cores(send1).astype(float32)).astype(bfloat16)
    dw1 = lax.all_to_all(dw1, plane, 0, 0, tiled=True)
    grad_first = jnp.sum(dw1.astype(float32), axis=0)

    dw2, dw3, grad_first = lax.optimization_barrier((dw2, dw3, grad_first))
    dw3 = dw3.reshape(2, half, half)
    dw3 = jnp.stack(in_order(dw3[0], dw3[1])).reshape(height, -1, half)
    dw3 = jnp.sum(lax.all_to_all(dw3, "y", 0, 0, tiled=True).astype(float32), axis=0)
    last = jnp.stack([dw2, dw3])
    low, high = jnp.split(last, 2, axis=1)
    other = swap_cores(jnp.where(first, high, low))
    grad_mid = jnp.concatenate(in_order(jnp.where(first, low, high), other), axis=2)

    sums = jnp.stack([gain_sum2, gain_sum3, bias_sum2, bias_sum3]).reshape(4, mp, half)
    mine = lax.dynamic_index_in_dim(sums, lane, axis=1, keepdims=False)
    later = jnp.concatenate(in_order(mine, swap_cores(mine)), axis=1)
    grad_gain = jnp.stack([gain_sum1, later[0], later[1]])
    grad_bias = jnp.stack([bias_sum1, later[2], later[3]])
    return (grad_first, grad_mid, grad_out, grad_gain, grad_bias)


def solution(mesh):
    grid = Mesh(mesh.devices.reshape(4, 4, 2, 4), ("z", "y", "c", "x"))
    return jax.shard_map(
        per_device,
        mesh=grid,
        in_specs=(
            P(rows_axes),
            P(),
            P(),
            P(),
            P(),
            P(None, "x"),
            P(None, None, "x"),
            P("x", None),
            P(None, "x"),
            P(None, "x"),
            P(rows_axes, None),
        ),
        out_specs=(
            P(rows_axes, "x"),
            P(None, rows_axes, "x"),
            P(("x", "z", "y", "c"), None),
            P(None, "x"),
            P(None, "x"),
        ),
        check_vma=False,
    )
```

```python
import math

import jax
import jax.numpy as jnp
from jax import lax
from jax.sharding import Mesh, PartitionSpec as P

epsilon_norm = 1e-05
plane = ("z", "y")
over_chips = (("z", "y", "x"),)
over_chips_x_last = (("z", "y"), "x")
over_rows = ("c", ("z", "y"))
rows_axes = ("z", "y", "c")
float32 = jnp.float32
bfloat16 = jnp.bfloat16


def swap_cores(array):
    return lax.ppermute(array, "c", [(0, 1), (1, 0)])


def from_everyone(array, axis):
    size = lax.axis_size(axis)
    return lax.all_to_all(
        jnp.broadcast_to(array[None], (size, *array.shape)), axis, 0, 0, tiled=True
    )


def sum_over(rows, stages):
    for axis in stages:
        if axis == "c":
            rows = rows + swap_cores(rows)
        else:
            rows = jnp.sum(from_everyone(rows, axis), axis=0)
    return rows[0]


def total_of(pair, stages):
    return jnp.split(sum_over(jnp.concatenate(pair)[None], stages), len(pair))


def float_mod(values, inverse, modulus):
    rest = values - jnp.floor(values * inverse) * modulus
    return jnp.where(rest >= modulus, rest - modulus, rest)


def encode(ids, hash_a, hash_b, hash_p, hash_m):
    modulus = hash_p.astype(float32)[None, :]
    buckets = hash_m.astype(float32)[None, :]
    below = 1.0 - 2.0**-21
    inverse_p = below / modulus
    inverse_m = below / buckets
    high = (hash_a // 128).astype(float32)[None, :]
    low = (hash_a % 128).astype(float32)[None, :]
    shift = hash_b.astype(float32)[None, :]
    step = 2.0 / (buckets - 1.0)
    reduced = float_mod(ids.astype(float32)[:, None], inverse_p, modulus)
    carried = float_mod(high * reduced, inverse_p, modulus)
    mixed = float_mod(carried * 128.0 + low * reduced + shift, inverse_p, modulus)
    hashed = float_mod(mixed, inverse_m, buckets)
    return lax.optimization_barrier((hashed * step - 1.0).astype(bfloat16))


def mish_act(values):
    power = jnp.exp(jnp.minimum(values, 30.0))
    ratio = power * (power + 2.0)
    return values * (ratio / (ratio + 2.0))


def mish_slope(values):
    power = jnp.exp(jnp.minimum(values, 30.0))
    ratio = power * (power + 2.0)
    inverse = 1.0 / (ratio + 2.0)
    return inverse * (ratio + 4.0 * values * (power * (power + 1.0)) * inverse)


def dot(left, right):
    return jnp.dot(left, right, preferred_element_type=float32)


def dot_rows(left, right):
    return lax.dot_general(left, right, (((0,), (0,)), ((), ())), preferred_element_type=float32)


def dot_back(left, right):
    return lax.dot_general(left, right, (((1,), (1,)), ((), ())), preferred_element_type=float32)


def normalise(summed, axis, batch_total):
    totals, squares = total_of((jnp.sum(summed, axis=0), jnp.sum(summed * summed, axis=0)), axis)
    average = totals / batch_total
    spread = squares / batch_total - average * average
    return average, 1.0 / jnp.sqrt(spread + epsilon_norm)


def flip_rows(array):
    half = array.shape[0] // 2
    return jnp.concatenate([array[half:], array[:half]])


def step(ids, hash_a, hash_b, hash_p, hash_m, w_in, w_mid, w_out, bn_gain, bn_bias, target):
    core = lax.axis_index("c")
    lane = lax.axis_index("x")
    first = core == 0
    mp = lax.axis_size("x")
    depth, height = lax.axis_size("z"), lax.axis_size("y")
    planes = depth * height
    rows, batch_devices = ids.shape[0], lax.axis_size(rows_axes)
    batch_total = rows * batch_devices
    width = w_in.shape[1]
    half = width // 2
    own = mp * half
    hidden = mp * width
    part = rows // mp
    out = w_out.shape[1]

    def in_order(mine, other):
        return jnp.where(first, mine, other), jnp.where(first, other, mine)

    def weight_part(layer, row, count):
        start = (layer, row, core * half)
        return lax.dynamic_slice(w_mid, start, (1, count, half)).reshape(count, half)

    w2_top = lax.all_gather(weight_part(0, 0, own), "x", axis=1, tiled=True)
    w2_near = weight_part(0, own, own)
    w2_far = [w2_near] + [
        lax.ppermute(w2_near, "x", [(i, i ^ k) for i in range(mp)]) for k in range(1, mp)
    ]
    w2_end = jnp.concatenate([lax.select_n(lane ^ k, *w2_far) for k in range(mp)], axis=1)
    w3_low, w3_high = jnp.split(weight_part(1, 0, hidden).reshape(mp, 2, half, half), 2, axis=1)
    w3_part = jnp.concatenate(in_order(w3_low, w3_high), axis=1).reshape(hidden, half)
    w3 = lax.all_gather(w3_part, "x", axis=1, tiled=True)

    def half_of(array, axis):
        return lax.dynamic_slice_in_dim(array, core * half, half, axis=axis)

    vectors = jnp.concatenate([half_of(bn_gain[1:], 1), half_of(bn_bias[1:], 1)])
    high = lax.reduce_precision(vectors, 8, 7)
    middle = lax.reduce_precision(vectors - high, 8, 7)
    low = vectors - high - middle
    small = jnp.concatenate(
        [
            half_of(w_out, 0).reshape(-1, width),
            jnp.concatenate([high, middle, low]).astype(bfloat16).reshape(-1, width),
        ]
    )
    small = jnp.pad(small, ((0, -small.shape[0] % 16), (0, 0)))
    target_own = lax.dynamic_slice_in_dim(target, lane * part, part, axis=0)
    wanted = jnp.concatenate([target_own, swap_cores(target_own)])

    encoded = encode(ids, hash_a, hash_b, hash_p, hash_m)
    z1 = dot(encoded, w_in)
    mean1, inv1 = normalise(z1, over_rows, batch_total)
    n1 = (z1 - mean1) * inv1
    a1 = bn_gain[0] * n1 + bn_bias[0]
    x1 = mish_act(a1).astype(bfloat16)
    message = jnp.concatenate(
        [x1.reshape(mp, part, width), jnp.broadcast_to(small[None], (mp, *small.shape))], axis=1
    )
    message = lax.all_to_all(message, "x", 0, 0, tiled=True)
    x1_own = jnp.concatenate(list(message[:, :part]), axis=1)
    x1_all = jnp.concatenate([x1_own, swap_cores(x1_own)])
    small = message[:, part:].reshape(mp, -1)
    w_out_own = small[:, : half * out].reshape(own, out)
    vectors = small[:, half * out : half * out + 12 * half].astype(float32)
    vectors = vectors.reshape(mp, 3, 4, half)
    vectors = vectors[:, 0] + vectors[:, 1] + vectors[:, 2]
    gain2, gain3, bias2, bias3 = vectors.transpose(1, 0, 2).reshape(4, own)
    z2 = dot(x1_all[:, :own], w2_top) + dot(x1_all[:, own:], w2_end)
    mean2, inv2 = normalise(z2, over_chips_x_last, batch_total)
    n2 = (z2 - mean2) * inv2
    a2 = gain2 * n2 + bias2
    x2 = mish_act(a2).astype(bfloat16)
    x2_other = swap_cores(flip_rows(x2))
    blocks = zip(jnp.split(x2, mp, axis=1), jnp.split(x2_other, mp, axis=1))
    x2_all = jnp.concatenate([block for pair in blocks for block in pair], axis=1)
    z3 = dot(x2_all, w3)
    mean3, inv3 = normalise(z3, over_chips, batch_total)
    n3 = (z3 - mean3) * inv3
    a3 = gain3 * n3 + bias3
    x3 = mish_act(a3).astype(bfloat16)

    y_part = dot(x3, w_out_own)
    predicted = y_part + swap_cores(flip_rows(y_part))
    g_y = ((predicted - wanted) / math.sqrt(batch_total)).astype(bfloat16)
    g_out = dot_rows(x3, g_y).reshape(mp, planes // 2, 2, -1, out)
    keep_out = jnp.where(first, g_out[:, :, 0], g_out[:, :, 1])
    send_out = jnp.where(first, g_out[:, :, 1], g_out[:, :, 0]).astype(bfloat16)
    keep_out = keep_out.astype(bfloat16)
    g_out = jnp.stack(in_order(keep_out, swap_cores(send_out)))
    g_out = g_out.transpose(0, 2, 1, 3, 4).reshape(depth, height * mp, -1)
    g_out = g_out.transpose(1, 0, 2).reshape(height * mp, 1, -1).astype(float32)

    u3 = dot_back(g_y, w_out_own)
    s3 = u3 * mish_slope(a3)
    bias_sum3, gain_sum3 = total_of((jnp.sum(s3, axis=0), jnp.sum(s3 * n3, axis=0)), over_chips)
    e3 = (gain3 * inv3 * (s3 - bias_sum3 / batch_total - n3 * gain_sum3 / batch_total)).astype(
        bfloat16
    )
    u2_part = jnp.split(dot_back(e3, w3), 2 * mp, axis=1)
    u2_send = jnp.concatenate(u2_part[1::2], axis=1).astype(bfloat16)
    u2 = jnp.concatenate(u2_part[::2], axis=1)
    u2 = u2 + swap_cores(flip_rows(u2_send)).astype(float32)
    dw3 = dot_rows(x2_all, e3).astype(bfloat16)
    dw3 = lax.psum_scatter(dw3, "z", scatter_dimension=0, tiled=True)
    dw3 = lax.psum_scatter(dw3, "x", scatter_dimension=1, tiled=True)

    s2 = u2 * mish_slope(a2)
    sums2 = jnp.concatenate([jnp.sum(s2, axis=0), jnp.sum(s2 * n2, axis=0)])
    count = sums2.shape[0]
    sums2 = jnp.broadcast_to(sums2[None, None], (height * mp, 1, count))
    sums2 = jnp.concatenate([sums2, g_out], axis=2)
    sums2 = jnp.sum(lax.all_to_all(sums2, ("y", "x"), 0, 0, tiled=True), axis=(0, 1))
    g_out = sums2[count:].reshape(depth, -1)
    sums2 = jnp.broadcast_to(sums2[None, :count], (depth, count))
    sums2 = jnp.concatenate([sums2, g_out], axis=1)[:, None]
    sums2 = jnp.sum(lax.all_to_all(sums2, "z", 0, 0, tiled=True), axis=(0, 1))
    bias_sum2, gain_sum2 = sums2[:own], sums2[own:count]
    grad_out = sums2[count:].reshape(-1, out)
    e2 = (gain2 * inv2 * (s2 - bias_sum2 / batch_total - n2 * gain_sum2 / batch_total)).astype(
        bfloat16
    )
    u1_send = [dot_back(e2[part:], w).astype(bfloat16) for w in (w2_top, w2_end)]
    u1_own = jnp.concatenate([dot_back(e2[:part], w) for w in (w2_top, w2_end)], axis=1)
    u1_send = swap_cores(jnp.concatenate(u1_send, axis=1))
    u1_own = (u1_own + u1_send.astype(float32)).astype(bfloat16)
    u1 = lax.all_to_all(u1_own, "x", 1, 0, tiled=True).astype(float32)
    dw2 = dot_rows(x1_all, e2).astype(bfloat16)
    dw2 = lax.psum_scatter(dw2, "z", scatter_dimension=0, tiled=True)
    dw2 = jnp.stack([b.reshape(height, -1, half) for b in jnp.split(dw2, mp, axis=1)], axis=1)
    dw2 = lax.all_to_all(dw2.reshape(height * mp, -1, half), ("y", "x"), 0, 0, tiled=True)
    dw2 = jnp.sum(dw2.astype(float32), axis=0)

    s1 = u1 * mish_slope(a1)
    bias_sum1, gain_sum1 = total_of((jnp.sum(s1, axis=0), jnp.sum(s1 * n1, axis=0)), over_rows)
    e1 = (
        bn_gain[0] * inv1 * (s1 - bias_sum1 / batch_total - n1 * gain_sum1 / batch_total)
    ).astype(bfloat16)
    dw1 = dot_rows(encoded, e1).reshape(planes, 2, -1, width)
    keep1 = jnp.where(first, dw1[:, 0], dw1[:, 1])
    send1 = jnp.where(first, dw1[:, 1], dw1[:, 0]).astype(bfloat16)
    dw1 = (keep1 + swap_cores(send1).astype(float32)).astype(bfloat16)
    dw1 = lax.all_to_all(dw1, plane, 0, 0, tiled=True)
    grad_first = jnp.sum(dw1.astype(float32), axis=0)

    dw2, dw3, grad_first = lax.optimization_barrier((dw2, dw3, grad_first))
    dw3 = dw3.reshape(2, half, half)
    dw3 = jnp.stack(in_order(dw3[0], dw3[1])).reshape(height, -1, half)
    dw3 = jnp.sum(lax.all_to_all(dw3, "y", 0, 0, tiled=True).astype(float32), axis=0)
    last = jnp.stack([dw2, dw3])
    low, high = jnp.split(last, 2, axis=1)
    other = swap_cores(jnp.where(first, high, low))
    grad_mid = jnp.concatenate(in_order(jnp.where(first, low, high), other), axis=2)

    sums = jnp.stack([gain_sum2, gain_sum3, bias_sum2, bias_sum3]).reshape(4, mp, half)
    mine = lax.dynamic_index_in_dim(sums, lane, axis=1, keepdims=False)
    later = jnp.concatenate(in_order(mine, swap_cores(mine)), axis=1)
    grad_gain = jnp.stack([gain_sum1, later[0], later[1]])
    grad_bias = jnp.stack([bias_sum1, later[2], later[3]])
    return (grad_first, grad_mid, grad_out, grad_gain, grad_bias)


def solution(mesh):
    grid = Mesh(mesh.devices.reshape(4, 4, 2, 4), ("z", "y", "c", "x"))
    return jax.shard_map(
        step,
        mesh=grid,
        in_specs=(
            P(rows_axes),
            P(),
            P(),
            P(),
            P(),
            P(None, "x"),
            P(None, None, "x"),
            P("x", None),
            P(None, "x"),
            P(None, "x"),
            P(rows_axes, None),
        ),
        out_specs=(
            P(rows_axes, "x"),
            P(None, rows_axes, "x"),
            P(("x", "z", "y", "c"), None),
            P(None, "x"),
            P(None, "x"),
        ),
        check_vma=False,
    )
```

```python
import math

import jax
import jax.numpy as jnp
from jax import lax
from jax.experimental import pallas as pl
from jax.sharding import Mesh, PartitionSpec as P

epsilon_norm = 1e-05
plane = ("z", "y")
over_chips = (("z", "y", "x"),)
over_chips_x_last = (("z", "y"), "x")
over_rows = ("c", ("z", "y"))
rows_axes = ("z", "y", "c")
float32 = jnp.float32
bfloat16 = jnp.bfloat16


def swap_cores(array):
    return lax.ppermute(array, "c", [(0, 1), (1, 0)])


def from_everyone(array, axis):
    size = lax.axis_size(axis)
    return lax.all_to_all(
        jnp.broadcast_to(array[None], (size, *array.shape)), axis, 0, 0, tiled=True
    )


def sum_over(rows, stages):
    for axis in stages:
        if axis == "c":
            rows = rows + swap_cores(rows)
        else:
            rows = jnp.sum(from_everyone(rows, axis), axis=0)
    return rows[0]


def total_of(pair, stages):
    return jnp.split(sum_over(jnp.concatenate(pair)[None], stages), len(pair))


def float_mod(values, inverse, modulus):
    rest = values - jnp.floor(values * inverse) * modulus
    return jnp.where(rest >= modulus, rest - modulus, rest)


def encode(ids, hash_a, hash_b, hash_p, hash_m):
    modulus = hash_p.astype(float32)[None, :]
    buckets = hash_m.astype(float32)[None, :]
    below = 1.0 - 2.0**-21
    inverse_p = below / modulus
    inverse_m = below / buckets
    high = (hash_a // 128).astype(float32)[None, :]
    low = (hash_a % 128).astype(float32)[None, :]
    shift = hash_b.astype(float32)[None, :]
    step = 2.0 / (buckets - 1.0)
    reduced = float_mod(ids.astype(float32)[:, None], inverse_p, modulus)
    carried = float_mod(high * reduced, inverse_p, modulus)
    mixed = float_mod(carried * 128.0 + low * reduced + shift, inverse_p, modulus)
    hashed = float_mod(mixed, inverse_m, buckets)
    return lax.optimization_barrier((hashed * step - 1.0).astype(bfloat16))


def mish_act(values):
    power = jnp.exp(jnp.minimum(values, 30.0))
    ratio = power * (power + 2.0)
    return values * (ratio / (ratio + 2.0))


def mish_slope(values):
    power = jnp.exp(jnp.minimum(values, 30.0))
    ratio = power * (power + 2.0)
    inverse = 1.0 / (ratio + 2.0)
    return inverse * (ratio + 4.0 * values * (power * (power + 1.0)) * inverse)


def dot(left, right):
    return jnp.dot(left, right, preferred_element_type=float32)


def dot_rows(left, right):
    return lax.dot_general(left, right, (((0,), (0,)), ((), ())), preferred_element_type=float32)


def dot_back(left, right):
    return lax.dot_general(left, right, (((1,), (1,)), ((), ())), preferred_element_type=float32)


def layer_dot(inputs, weights):
    rows, width = inputs.shape[0], weights[0].shape[1]
    block = min(256, width)

    def body(input_ref, *refs):
        product = 0.0
        start = 0
        for ref in refs[:-2]:
            end = start + ref.shape[0]
            product = product + dot(input_ref[:, start:end], ref[...])
            start = end
        refs[-2][...] = product
        refs[-1][0:1, :] = jnp.sum(product, axis=0, keepdims=True)
        refs[-1][1:2, :] = jnp.sum(product * product, axis=0, keepdims=True)

    return pl.pallas_call(
        body,
        grid=(width // block,),
        in_specs=[pl.BlockSpec(inputs.shape, lambda n: (0, 0))]
        + [pl.BlockSpec((w.shape[0], block), lambda n: (0, n)) for w in weights],
        out_specs=[
            pl.BlockSpec((rows, block), lambda n: (0, n)),
            pl.BlockSpec((2, block), lambda n: (0, n)),
        ],
        out_shape=[
            jax.ShapeDtypeStruct((rows, width), float32),
            jax.ShapeDtypeStruct((2, width), float32),
        ],
        cost_estimate=pl.CostEstimate(
            flops=2 * rows * inputs.shape[1] * width,
            transcendentals=0,
            bytes_accessed=2 * inputs.size + 2 * inputs.shape[1] * width + 4 * rows * width,
        ),
    )(inputs, *weights)


def back_dot(slopes, weights, half):
    rows, width = slopes.shape
    middle = rows // 2

    def body(slope_ref, weight_ref, keep_ref, send_ref):
        product = dot_back(slope_ref[...], weight_ref[...])
        keep_ref[...] = product[:, :half]
        send_ref[:middle, :] = product[middle:, half:].astype(bfloat16)
        send_ref[middle:, :] = product[:middle, half:].astype(bfloat16)

    units = weights.shape[0] // 2
    return pl.pallas_call(
        body,
        grid=(units // half,),
        in_specs=[
            pl.BlockSpec(slopes.shape, lambda n: (0, 0)),
            pl.BlockSpec((2 * half, width), lambda n: (n, 0)),
        ],
        out_specs=[
            pl.BlockSpec((rows, half), lambda n: (0, n)),
            pl.BlockSpec((rows, half), lambda n: (0, n)),
        ],
        out_shape=[
            jax.ShapeDtypeStruct((rows, units), float32),
            jax.ShapeDtypeStruct((rows, units), bfloat16),
        ],
        cost_estimate=pl.CostEstimate(
            flops=4 * rows * width * units,
            transcendentals=0,
            bytes_accessed=2 * slopes.size + 2 * weights.size + 6 * rows * units,
        ),
    )(slopes, weights)


def normalise(sums, axis, batch_total):
    totals, squares = total_of(sums, axis)
    average = totals / batch_total
    spread = squares / batch_total - average * average
    return average, 1.0 / jnp.sqrt(spread + epsilon_norm)


def flip_rows(array):
    half = array.shape[0] // 2
    return jnp.concatenate([array[half:], array[:half]])


def step(ids, hash_a, hash_b, hash_p, hash_m, w_in, w_mid, w_out, bn_gain, bn_bias, target):
    core = lax.axis_index("c")
    lane = lax.axis_index("x")
    first = core == 0
    mp = lax.axis_size("x")
    depth, height = lax.axis_size("z"), lax.axis_size("y")
    planes = depth * height
    rows, batch_devices = ids.shape[0], lax.axis_size(rows_axes)
    batch_total = rows * batch_devices
    width = w_in.shape[1]
    half = width // 2
    own = mp * half
    hidden = mp * width
    part = rows // mp
    out = w_out.shape[1]

    def in_order(mine, other):
        return jnp.where(first, mine, other), jnp.where(first, other, mine)

    def weight_part(layer, row, count):
        start = (layer, row, core * half)
        return lax.dynamic_slice(w_mid, start, (1, count, half)).reshape(count, half)

    w2_top = lax.all_gather(weight_part(0, 0, own), "x", axis=1, tiled=True)
    w2_near = weight_part(0, own, own)
    w2_far = [w2_near] + [
        lax.ppermute(w2_near, "x", [(i, i ^ k) for i in range(mp)]) for k in range(1, mp)
    ]
    w2_end = jnp.concatenate([lax.select_n(lane ^ k, *w2_far) for k in range(mp)], axis=1)
    w3_low, w3_high = jnp.split(weight_part(1, 0, hidden).reshape(mp, 2, half, half), 2, axis=1)
    w3_part = jnp.concatenate(in_order(w3_low, w3_high), axis=1).reshape(hidden, half)
    w3 = lax.all_gather(w3_part, "x", axis=1, tiled=True)

    def half_of(array, axis):
        return lax.dynamic_slice_in_dim(array, core * half, half, axis=axis)

    vectors = jnp.concatenate([half_of(bn_gain[1:], 1), half_of(bn_bias[1:], 1)])
    high = lax.reduce_precision(vectors, 8, 7)
    middle = lax.reduce_precision(vectors - high, 8, 7)
    low = vectors - high - middle
    small = jnp.concatenate(
        [
            half_of(w_out, 0).reshape(-1, width),
            jnp.concatenate([high, middle, low]).astype(bfloat16).reshape(-1, width),
        ]
    )
    small = jnp.pad(small, ((0, -small.shape[0] % 16), (0, 0)))
    target_own = lax.dynamic_slice_in_dim(target, lane * part, part, axis=0)
    wanted = jnp.concatenate([target_own, swap_cores(target_own)])

    encoded = encode(ids, hash_a, hash_b, hash_p, hash_m)
    z1 = dot(encoded, w_in)
    sums1 = (jnp.sum(z1, axis=0), jnp.sum(z1 * z1, axis=0))
    mean1, inv1 = normalise(sums1, over_rows, batch_total)
    n1 = (z1 - mean1) * inv1
    a1 = bn_gain[0] * n1 + bn_bias[0]
    x1 = mish_act(a1).astype(bfloat16)
    message = jnp.concatenate(
        [x1.reshape(mp, part, width), jnp.broadcast_to(small[None], (mp, *small.shape))], axis=1
    )
    message = lax.all_to_all(message, "x", 0, 0, tiled=True)
    x1_own = jnp.concatenate(list(message[:, :part]), axis=1)
    x1_all = jnp.concatenate([x1_own, swap_cores(x1_own)])
    small = message[:, part:].reshape(mp, -1)
    w_out_own = small[:, : half * out].reshape(own, out)
    vectors = small[:, half * out : half * out + 12 * half].astype(float32)
    vectors = vectors.reshape(mp, 3, 4, half)
    vectors = vectors[:, 0] + vectors[:, 1] + vectors[:, 2]
    gain2, gain3, bias2, bias3 = vectors.transpose(1, 0, 2).reshape(4, own)
    z2, sums2 = layer_dot(x1_all, (w2_top, w2_end))
    mean2, inv2 = normalise((sums2[0], sums2[1]), over_chips_x_last, batch_total)
    n2 = (z2 - mean2) * inv2
    a2 = gain2 * n2 + bias2
    x2 = mish_act(a2).astype(bfloat16)
    x2_other = swap_cores(flip_rows(x2))
    blocks = zip(jnp.split(x2, mp, axis=1), jnp.split(x2_other, mp, axis=1))
    x2_all = jnp.concatenate([block for pair in blocks for block in pair], axis=1)
    z3, sums3 = layer_dot(x2_all, (w3,))
    mean3, inv3 = normalise((sums3[0], sums3[1]), over_chips, batch_total)
    n3 = (z3 - mean3) * inv3
    a3 = gain3 * n3 + bias3
    x3 = mish_act(a3).astype(bfloat16)

    y_part = dot(x3, w_out_own)
    predicted = y_part + swap_cores(flip_rows(y_part))
    g_y = ((predicted - wanted) / math.sqrt(batch_total)).astype(bfloat16)
    g_out = dot_rows(x3, g_y).reshape(mp, planes // 2, 2, -1, out)
    keep_out = jnp.where(first, g_out[:, :, 0], g_out[:, :, 1])
    send_out = jnp.where(first, g_out[:, :, 1], g_out[:, :, 0]).astype(bfloat16)
    keep_out = keep_out.astype(bfloat16)
    g_out = jnp.stack(in_order(keep_out, swap_cores(send_out)))
    g_out = g_out.transpose(0, 2, 1, 3, 4).reshape(depth, height * mp, -1)
    g_out = g_out.transpose(1, 0, 2).reshape(height * mp, 1, -1).astype(float32)

    u3 = dot_back(g_y, w_out_own)
    s3 = u3 * mish_slope(a3)
    bias_sum3, gain_sum3 = total_of((jnp.sum(s3, axis=0), jnp.sum(s3 * n3, axis=0)), over_chips)
    e3 = (gain3 * inv3 * (s3 - bias_sum3 / batch_total - n3 * gain_sum3 / batch_total)).astype(
        bfloat16
    )
    u2_keep, u2_send = back_dot(e3, w3, half)
    u2 = u2_keep + swap_cores(u2_send).astype(float32)
    dw3 = dot_rows(x2_all, e3).astype(bfloat16)
    dw3 = lax.psum_scatter(dw3, "z", scatter_dimension=0, tiled=True)
    dw3 = lax.psum_scatter(dw3, "x", scatter_dimension=1, tiled=True)

    s2 = u2 * mish_slope(a2)
    sums2 = jnp.concatenate([jnp.sum(s2, axis=0), jnp.sum(s2 * n2, axis=0)])
    count = sums2.shape[0]
    sums2 = jnp.broadcast_to(sums2[None, None], (height * mp, 1, count))
    sums2 = jnp.concatenate([sums2, g_out], axis=2)
    sums2 = jnp.sum(lax.all_to_all(sums2, ("y", "x"), 0, 0, tiled=True), axis=(0, 1))
    g_out = sums2[count:].reshape(depth, -1)
    sums2 = jnp.broadcast_to(sums2[None, :count], (depth, count))
    sums2 = jnp.concatenate([sums2, g_out], axis=1)[:, None]
    sums2 = jnp.sum(lax.all_to_all(sums2, "z", 0, 0, tiled=True), axis=(0, 1))
    bias_sum2, gain_sum2 = sums2[:own], sums2[own:count]
    grad_out = sums2[count:].reshape(-1, out)
    e2 = (gain2 * inv2 * (s2 - bias_sum2 / batch_total - n2 * gain_sum2 / batch_total)).astype(
        bfloat16
    )
    u1_send = [dot_back(e2[part:], w).astype(bfloat16) for w in (w2_top, w2_end)]
    u1_own = jnp.concatenate([dot_back(e2[:part], w) for w in (w2_top, w2_end)], axis=1)
    u1_send = swap_cores(jnp.concatenate(u1_send, axis=1))
    u1_own = (u1_own + u1_send.astype(float32)).astype(bfloat16)
    u1 = lax.all_to_all(u1_own, "x", 1, 0, tiled=True).astype(float32)
    dw2 = dot_rows(x1_all, e2).astype(bfloat16)
    dw2 = lax.psum_scatter(dw2, "z", scatter_dimension=0, tiled=True)
    dw2 = jnp.stack([b.reshape(height, -1, half) for b in jnp.split(dw2, mp, axis=1)], axis=1)
    dw2 = lax.all_to_all(dw2.reshape(height * mp, -1, half), ("y", "x"), 0, 0, tiled=True)
    dw2 = jnp.sum(dw2.astype(float32), axis=0)

    s1 = u1 * mish_slope(a1)
    bias_sum1, gain_sum1 = total_of((jnp.sum(s1, axis=0), jnp.sum(s1 * n1, axis=0)), over_rows)
    e1 = (
        bn_gain[0] * inv1 * (s1 - bias_sum1 / batch_total - n1 * gain_sum1 / batch_total)
    ).astype(bfloat16)
    dw1 = dot_rows(encoded, e1).reshape(planes, 2, -1, width)
    keep1 = jnp.where(first, dw1[:, 0], dw1[:, 1])
    send1 = jnp.where(first, dw1[:, 1], dw1[:, 0]).astype(bfloat16)
    dw1 = (keep1 + swap_cores(send1).astype(float32)).astype(bfloat16)
    dw1 = lax.all_to_all(dw1, plane, 0, 0, tiled=True)
    grad_first = jnp.sum(dw1.astype(float32), axis=0)

    dw2, dw3, grad_first = lax.optimization_barrier((dw2, dw3, grad_first))
    dw3 = dw3.reshape(2, half, half)
    dw3 = jnp.stack(in_order(dw3[0], dw3[1])).reshape(height, -1, half)
    dw3 = jnp.sum(lax.all_to_all(dw3, "y", 0, 0, tiled=True).astype(float32), axis=0)
    last = jnp.stack([dw2, dw3])
    low, high = jnp.split(last, 2, axis=1)
    other = swap_cores(jnp.where(first, high, low))
    grad_mid = jnp.concatenate(in_order(jnp.where(first, low, high), other), axis=2)

    sums = jnp.stack([gain_sum2, gain_sum3, bias_sum2, bias_sum3]).reshape(4, mp, half)
    mine = lax.dynamic_index_in_dim(sums, lane, axis=1, keepdims=False)
    later = jnp.concatenate(in_order(mine, swap_cores(mine)), axis=1)
    grad_gain = jnp.stack([gain_sum1, later[0], later[1]])
    grad_bias = jnp.stack([bias_sum1, later[2], later[3]])
    return (grad_first, grad_mid, grad_out, grad_gain, grad_bias)


def solution(mesh):
    grid = Mesh(mesh.devices.reshape(4, 4, 2, 4), ("z", "y", "c", "x"))
    return jax.shard_map(
        step,
        mesh=grid,
        in_specs=(
            P(rows_axes),
            P(),
            P(),
            P(),
            P(),
            P(None, "x"),
            P(None, None, "x"),
            P("x", None),
            P(None, "x"),
            P(None, "x"),
            P(rows_axes, None),
        ),
        out_specs=(
            P(rows_axes, "x"),
            P(None, rows_axes, "x"),
            P(("x", "z", "y", "c"), None),
            P(None, "x"),
            P(None, "x"),
        ),
        check_vma=False,
    )
```

```python
import math

import jax
import jax.numpy as jnp
from jax import lax
from jax.experimental import pallas as pl
from jax.sharding import Mesh, PartitionSpec as P

epsilon_norm = 1e-05
plane = ("z", "y")
over_chips = (("z", "y", "x"),)
over_chips_x_last = (("z", "y"), "x")
over_rows = ("c", ("z", "y"))
rows_axes = ("z", "y", "c")
float32 = jnp.float32
bfloat16 = jnp.bfloat16


def swap_cores(array):
    return lax.ppermute(array, "c", [(0, 1), (1, 0)])


def from_everyone(array, axis):
    size = lax.axis_size(axis)
    return lax.all_to_all(
        jnp.broadcast_to(array[None], (size, *array.shape)), axis, 0, 0, tiled=True
    )


def sum_over(rows, stages):
    for axis in stages:
        if axis == "c":
            rows = rows + swap_cores(rows)
        else:
            rows = jnp.sum(from_everyone(rows, axis), axis=0)
    return rows[0]


def total_of(pair, stages):
    return jnp.split(sum_over(jnp.concatenate(pair)[None], stages), len(pair))


def float_mod(values, inverse, modulus):
    rest = values - jnp.floor(values * inverse) * modulus
    return jnp.where(rest >= modulus, rest - modulus, rest)


def encode(ids, hash_a, hash_b, hash_p, hash_m):
    modulus = hash_p.astype(float32)[None, :]
    buckets = hash_m.astype(float32)[None, :]
    below = 1.0 - 2.0**-21
    inverse_p = below / modulus
    inverse_m = below / buckets
    high = (hash_a // 128).astype(float32)[None, :]
    low = (hash_a % 128).astype(float32)[None, :]
    shift = hash_b.astype(float32)[None, :]
    step = 2.0 / (buckets - 1.0)
    reduced = float_mod(ids.astype(float32)[:, None], inverse_p, modulus)
    carried = float_mod(high * reduced, inverse_p, modulus)
    mixed = float_mod(carried * 128.0 + low * reduced + shift, inverse_p, modulus)
    hashed = float_mod(mixed, inverse_m, buckets)
    return lax.optimization_barrier((hashed * step - 1.0).astype(bfloat16))


def mish_act(values):
    power = jnp.exp(jnp.minimum(values, 30.0))
    ratio = power * (power + 2.0)
    return values * (ratio / (ratio + 2.0))


def mish_slope(values):
    power = jnp.exp(jnp.minimum(values, 30.0))
    ratio = power * (power + 2.0)
    inverse = 1.0 / (ratio + 2.0)
    return inverse * (ratio + 4.0 * values * (power * (power + 1.0)) * inverse)


def dot(left, right):
    return jnp.dot(left, right, preferred_element_type=float32)


def dot_rows(left, right):
    return lax.dot_general(left, right, (((0,), (0,)), ((), ())), preferred_element_type=float32)


def dot_back(left, right):
    return lax.dot_general(left, right, (((1,), (1,)), ((), ())), preferred_element_type=float32)


def layer_dot(inputs, weights):
    part, units = inputs[0].shape
    rows, width = part * len(inputs), weights[0].shape[1]
    block = min(256, width)

    def body(*refs):
        input_refs, weight_refs = refs[: len(inputs)], refs[len(inputs) : -2]
        totals, squares = 0.0, 0.0
        for at, input_ref in enumerate(input_refs):
            product = 0.0
            start = 0
            for ref in weight_refs:
                end = start + ref.shape[0]
                product = product + dot(input_ref[:, start:end], ref[...])
                start = end
            refs[-2][at * part : (at + 1) * part, :] = product
            totals = totals + jnp.sum(product, axis=0, keepdims=True)
            squares = squares + jnp.sum(product * product, axis=0, keepdims=True)
        refs[-1][0:1, :] = totals
        refs[-1][1:2, :] = squares

    return pl.pallas_call(
        body,
        grid=(width // block,),
        in_specs=[pl.BlockSpec((part, units), lambda n: (0, 0)) for _ in inputs]
        + [pl.BlockSpec((w.shape[0], block), lambda n: (0, n)) for w in weights],
        out_specs=[
            pl.BlockSpec((rows, block), lambda n: (0, n)),
            pl.BlockSpec((2, block), lambda n: (0, n)),
        ],
        out_shape=[
            jax.ShapeDtypeStruct((rows, width), float32),
            jax.ShapeDtypeStruct((2, width), float32),
        ],
        cost_estimate=pl.CostEstimate(
            flops=2 * rows * units * width,
            transcendentals=0,
            bytes_accessed=2 * rows * units + 2 * units * width + 4 * rows * width,
        ),
    )(*inputs, *weights)


def back_dot(slopes, weights, half):
    rows, width = slopes.shape
    middle = rows // 2

    def body(slope_ref, weight_ref, keep_ref, send_ref):
        product = dot_back(slope_ref[...], weight_ref[...])
        keep_ref[...] = product[:, :half]
        send_ref[:middle, :] = product[middle:, half:].astype(bfloat16)
        send_ref[middle:, :] = product[:middle, half:].astype(bfloat16)

    units = weights.shape[0] // 2
    return pl.pallas_call(
        body,
        grid=(units // half,),
        in_specs=[
            pl.BlockSpec(slopes.shape, lambda n: (0, 0)),
            pl.BlockSpec((2 * half, width), lambda n: (n, 0)),
        ],
        out_specs=[
            pl.BlockSpec((rows, half), lambda n: (0, n)),
            pl.BlockSpec((rows, half), lambda n: (0, n)),
        ],
        out_shape=[
            jax.ShapeDtypeStruct((rows, units), float32),
            jax.ShapeDtypeStruct((rows, units), bfloat16),
        ],
        cost_estimate=pl.CostEstimate(
            flops=4 * rows * width * units,
            transcendentals=0,
            bytes_accessed=2 * slopes.size + 2 * weights.size + 6 * rows * units,
        ),
    )(slopes, weights)


def normalise(sums, axis, batch_total):
    totals, squares = total_of(sums, axis)
    average = totals / batch_total
    spread = squares / batch_total - average * average
    return average, 1.0 / jnp.sqrt(spread + epsilon_norm)


def flip_rows(array):
    half = array.shape[0] // 2
    return jnp.concatenate([array[half:], array[:half]])


def step(ids, hash_a, hash_b, hash_p, hash_m, w_in, w_mid, w_out, bn_gain, bn_bias, target):
    core = lax.axis_index("c")
    lane = lax.axis_index("x")
    first = core == 0
    mp = lax.axis_size("x")
    depth, height = lax.axis_size("z"), lax.axis_size("y")
    planes = depth * height
    rows, batch_devices = ids.shape[0], lax.axis_size(rows_axes)
    batch_total = rows * batch_devices
    width = w_in.shape[1]
    half = width // 2
    own = mp * half
    hidden = mp * width
    part = rows // mp
    out = w_out.shape[1]

    def in_order(mine, other):
        return jnp.where(first, mine, other), jnp.where(first, other, mine)

    def weight_part(layer, row, count):
        start = (layer, row, core * half)
        return lax.dynamic_slice(w_mid, start, (1, count, half)).reshape(count, half)

    w2_top = lax.all_gather(weight_part(0, 0, own), "x", axis=1, tiled=True)
    w2_near = weight_part(0, own, own)
    w2_far = [w2_near] + [
        lax.ppermute(w2_near, "x", [(i, i ^ k) for i in range(mp)]) for k in range(1, mp)
    ]
    w2_end = jnp.concatenate([lax.select_n(lane ^ k, *w2_far) for k in range(mp)], axis=1)
    w3_low, w3_high = jnp.split(weight_part(1, 0, hidden).reshape(mp, 2, half, half), 2, axis=1)
    w3_part = jnp.concatenate(in_order(w3_low, w3_high), axis=1).reshape(hidden, half)
    w3 = lax.all_gather(w3_part, "x", axis=1, tiled=True)

    def half_of(array, axis):
        return lax.dynamic_slice_in_dim(array, core * half, half, axis=axis)

    vectors = jnp.concatenate([half_of(bn_gain[1:], 1), half_of(bn_bias[1:], 1)])
    high = lax.reduce_precision(vectors, 8, 7)
    middle = lax.reduce_precision(vectors - high, 8, 7)
    low = vectors - high - middle
    small = jnp.concatenate(
        [
            half_of(w_out, 0).reshape(-1, width),
            jnp.concatenate([high, middle, low]).astype(bfloat16).reshape(-1, width),
        ]
    )
    small = jnp.pad(small, ((0, -small.shape[0] % 16), (0, 0)))
    target_own = lax.dynamic_slice_in_dim(target, lane * part, part, axis=0)
    wanted = jnp.concatenate([target_own, swap_cores(target_own)])

    encoded = encode(ids, hash_a, hash_b, hash_p, hash_m)
    z1 = dot(encoded, w_in)
    sums1 = (jnp.sum(z1, axis=0), jnp.sum(z1 * z1, axis=0))
    mean1, inv1 = normalise(sums1, over_rows, batch_total)
    n1 = (z1 - mean1) * inv1
    a1 = bn_gain[0] * n1 + bn_bias[0]
    x1 = mish_act(a1).astype(bfloat16)
    message = jnp.concatenate(
        [x1.reshape(mp, part, width), jnp.broadcast_to(small[None], (mp, *small.shape))], axis=1
    )
    message = lax.all_to_all(message, "x", 0, 0, tiled=True)
    x1_own = jnp.concatenate(list(message[:, :part]), axis=1)
    x1_other = swap_cores(x1_own)
    x1_all = jnp.concatenate([x1_own, x1_other])
    small = message[:, part:].reshape(mp, -1)
    w_out_own = small[:, : half * out].reshape(own, out)
    vectors = small[:, half * out : half * out + 12 * half].astype(float32)
    vectors = vectors.reshape(mp, 3, 4, half)
    vectors = vectors[:, 0] + vectors[:, 1] + vectors[:, 2]
    gain2, gain3, bias2, bias3 = vectors.transpose(1, 0, 2).reshape(4, own)
    z2, sums2 = layer_dot((x1_own, x1_other), (w2_top, w2_end))
    mean2, inv2 = normalise((sums2[0], sums2[1]), over_chips_x_last, batch_total)
    n2 = (z2 - mean2) * inv2
    a2 = gain2 * n2 + bias2
    x2 = mish_act(a2).astype(bfloat16)
    x2_other = swap_cores(flip_rows(x2))
    blocks = zip(jnp.split(x2, mp, axis=1), jnp.split(x2_other, mp, axis=1))
    x2_all = jnp.concatenate([block for pair in blocks for block in pair], axis=1)
    z3, sums3 = layer_dot((x2_all,), (w3,))
    mean3, inv3 = normalise((sums3[0], sums3[1]), over_chips, batch_total)
    n3 = (z3 - mean3) * inv3
    a3 = gain3 * n3 + bias3
    x3 = mish_act(a3).astype(bfloat16)

    y_part = dot(x3, w_out_own)
    predicted = y_part + swap_cores(flip_rows(y_part))
    g_y = ((predicted - wanted) / math.sqrt(batch_total)).astype(bfloat16)
    g_out = dot_rows(x3, g_y).reshape(mp, planes // 2, 2, -1, out)
    keep_out = jnp.where(first, g_out[:, :, 0], g_out[:, :, 1])
    send_out = jnp.where(first, g_out[:, :, 1], g_out[:, :, 0]).astype(bfloat16)
    keep_out = keep_out.astype(bfloat16)
    g_out = jnp.stack(in_order(keep_out, swap_cores(send_out)))
    g_out = g_out.transpose(0, 2, 1, 3, 4).reshape(depth, height * mp, -1)
    g_out = g_out.transpose(1, 0, 2).reshape(height * mp, 1, -1).astype(float32)

    u3 = dot_back(g_y, w_out_own)
    s3 = u3 * mish_slope(a3)
    bias_sum3, gain_sum3 = total_of((jnp.sum(s3, axis=0), jnp.sum(s3 * n3, axis=0)), over_chips)
    e3 = (gain3 * inv3 * (s3 - bias_sum3 / batch_total - n3 * gain_sum3 / batch_total)).astype(
        bfloat16
    )
    u2_keep, u2_send = back_dot(e3, w3, half)
    u2 = u2_keep + swap_cores(u2_send).astype(float32)
    dw3 = dot_rows(x2_all, e3).astype(bfloat16)
    dw3 = lax.psum_scatter(dw3, "z", scatter_dimension=0, tiled=True)
    dw3_low, dw3_high = jnp.split(dw3, 2)
    dw3 = jnp.concatenate(in_order(dw3_low, dw3_high))
    dw3 = lax.psum_scatter(dw3, "x", scatter_dimension=1, tiled=True)
    dw3 = lax.psum_scatter(dw3, "y", scatter_dimension=0, tiled=True).astype(float32)

    s2 = u2 * mish_slope(a2)
    sums2 = jnp.concatenate([jnp.sum(s2, axis=0), jnp.sum(s2 * n2, axis=0)])
    count = sums2.shape[0]
    sums2 = jnp.broadcast_to(sums2[None, None], (height * mp, 1, count))
    sums2 = jnp.concatenate([sums2, g_out], axis=2)
    sums2 = jnp.sum(lax.all_to_all(sums2, ("y", "x"), 0, 0, tiled=True), axis=(0, 1))
    g_out = sums2[count:].reshape(depth, -1)
    sums2 = jnp.broadcast_to(sums2[None, :count], (depth, count))
    sums2 = jnp.concatenate([sums2, g_out], axis=1)[:, None]
    sums2 = jnp.sum(lax.all_to_all(sums2, "z", 0, 0, tiled=True), axis=(0, 1))
    bias_sum2, gain_sum2 = sums2[:own], sums2[own:count]
    grad_out = sums2[count:].reshape(-1, out)
    e2 = (gain2 * inv2 * (s2 - bias_sum2 / batch_total - n2 * gain_sum2 / batch_total)).astype(
        bfloat16
    )
    u1_send = [dot_back(e2[part:], w).astype(bfloat16) for w in (w2_top, w2_end)]
    u1_own = jnp.concatenate([dot_back(e2[:part], w) for w in (w2_top, w2_end)], axis=1)
    u1_send = swap_cores(jnp.concatenate(u1_send, axis=1))
    u1_own = (u1_own + u1_send.astype(float32)).astype(bfloat16)
    u1 = lax.all_to_all(u1_own, "x", 1, 0, tiled=True).astype(float32)
    dw2 = dot_rows(x1_all, e2).astype(bfloat16)
    dw2 = lax.psum_scatter(dw2, "z", scatter_dimension=0, tiled=True)
    dw2 = jnp.stack([b.reshape(height, -1, half) for b in jnp.split(dw2, mp, axis=1)], axis=1)
    dw2 = lax.all_to_all(dw2.reshape(height * mp, -1, half), ("y", "x"), 0, 0, tiled=True)
    dw2 = jnp.sum(dw2.astype(float32), axis=0)

    s1 = u1 * mish_slope(a1)
    bias_sum1, gain_sum1 = total_of((jnp.sum(s1, axis=0), jnp.sum(s1 * n1, axis=0)), over_rows)
    e1 = (
        bn_gain[0] * inv1 * (s1 - bias_sum1 / batch_total - n1 * gain_sum1 / batch_total)
    ).astype(bfloat16)
    dw1 = dot_rows(encoded, e1).reshape(planes, 2, -1, width)
    keep1 = jnp.where(first, dw1[:, 0], dw1[:, 1])
    send1 = jnp.where(first, dw1[:, 1], dw1[:, 0]).astype(bfloat16)
    dw1 = (keep1 + swap_cores(send1).astype(float32)).astype(bfloat16)
    dw1 = lax.all_to_all(dw1, plane, 0, 0, tiled=True)
    grad_first = jnp.sum(dw1.astype(float32), axis=0)

    last = jnp.stack([dw2, dw3])
    low, high = jnp.split(last, 2, axis=1)
    other = swap_cores(jnp.where(first, high, low))
    grad_mid = jnp.concatenate(in_order(jnp.where(first, low, high), other), axis=2)

    sums = jnp.stack([gain_sum2, gain_sum3, bias_sum2, bias_sum3]).reshape(4, mp, half)
    mine = lax.dynamic_index_in_dim(sums, lane, axis=1, keepdims=False)
    later = jnp.concatenate(in_order(mine, swap_cores(mine)), axis=1)
    grad_gain = jnp.stack([gain_sum1, later[0], later[1]])
    grad_bias = jnp.stack([bias_sum1, later[2], later[3]])
    return (grad_first, grad_mid, grad_out, grad_gain, grad_bias)


def solution(mesh):
    grid = Mesh(mesh.devices.reshape(4, 4, 2, 4), ("z", "y", "c", "x"))
    return jax.shard_map(
        step,
        mesh=grid,
        in_specs=(
            P(rows_axes),
            P(),
            P(),
            P(),
            P(),
            P(None, "x"),
            P(None, None, "x"),
            P("x", None),
            P(None, "x"),
            P(None, "x"),
            P(rows_axes, None),
        ),
        out_specs=(
            P(rows_axes, "x"),
            P(None, rows_axes, "x"),
            P(("x", "z", "y", "c"), None),
            P(None, "x"),
            P(None, "x"),
        ),
        check_vma=False,
    )
```

```python
import math

import jax
import jax.numpy as jnp
from jax import lax
from jax.experimental import pallas as pl
from jax.sharding import Mesh, PartitionSpec as P

epsilon_norm = 1e-05
plane = ("z", "y")
over_chips = (("z", "y", "x"),)
over_chips_x_last = (("z", "y"), "x")
over_rows = ("c", ("z", "y"))
rows_axes = ("z", "y", "c")
float32 = jnp.float32
bfloat16 = jnp.bfloat16


def swap_cores(array):
    return lax.ppermute(array, "c", [(0, 1), (1, 0)])


def from_everyone(array, axis):
    size = lax.axis_size(axis)
    return lax.all_to_all(
        jnp.broadcast_to(array[None], (size, *array.shape)), axis, 0, 0, tiled=True
    )


def sum_over(rows, stages):
    for axis in stages:
        if axis == "c":
            rows = rows + swap_cores(rows)
        else:
            rows = jnp.sum(from_everyone(rows, axis), axis=0)
    return rows[0]


def total_of(pair, stages):
    return jnp.split(sum_over(jnp.concatenate(pair)[None], stages), len(pair))


def float_mod(values, inverse, modulus):
    rest = values - jnp.floor(values * inverse) * modulus
    return jnp.where(rest >= modulus, rest - modulus, rest)


def encode(ids, hash_a, hash_b, hash_p, hash_m):
    modulus = hash_p.astype(float32)[None, :]
    buckets = hash_m.astype(float32)[None, :]
    below = 1.0 - 2.0**-21
    inverse_p = below / modulus
    inverse_m = below / buckets
    high = (hash_a // 128).astype(float32)[None, :]
    low = (hash_a % 128).astype(float32)[None, :]
    shift = hash_b.astype(float32)[None, :]
    step = 2.0 / (buckets - 1.0)
    reduced = float_mod(ids.astype(float32)[:, None], inverse_p, modulus)
    carried = float_mod(high * reduced, inverse_p, modulus)
    mixed = float_mod(carried * 128.0 + low * reduced + shift, inverse_p, modulus)
    hashed = float_mod(mixed, inverse_m, buckets)
    return lax.optimization_barrier((hashed * step - 1.0).astype(bfloat16))


def mish_act(values):
    power = jnp.exp(jnp.minimum(values, 30.0))
    ratio = power * (power + 2.0)
    return values * (ratio / (ratio + 2.0))


def mish_slope(values):
    power = jnp.exp(jnp.minimum(values, 30.0))
    ratio = power * (power + 2.0)
    inverse = 1.0 / (ratio + 2.0)
    return inverse * (ratio + 4.0 * values * (power * (power + 1.0)) * inverse)


def dot(left, right):
    return jnp.dot(left, right, preferred_element_type=float32)


def dot_rows(left, right):
    return lax.dot_general(left, right, (((0,), (0,)), ((), ())), preferred_element_type=float32)


def dot_back(left, right):
    return lax.dot_general(left, right, (((1,), (1,)), ((), ())), preferred_element_type=float32)


def layer_dot(inputs, weights):
    part, units = inputs[0].shape
    rows, width = part * len(inputs), weights[0].shape[1]
    block = min(256, width)

    def body(*refs):
        input_refs, weight_refs = refs[: len(inputs)], refs[len(inputs) : -2]
        totals, squares = 0.0, 0.0
        for at, input_ref in enumerate(input_refs):
            product = 0.0
            start = 0
            for ref in weight_refs:
                end = start + ref.shape[0]
                product = product + dot(input_ref[:, start:end], ref[...])
                start = end
            refs[-2][at * part : (at + 1) * part, :] = product
            totals = totals + jnp.sum(product, axis=0, keepdims=True)
            squares = squares + jnp.sum(product * product, axis=0, keepdims=True)
        refs[-1][0:1, :] = totals
        refs[-1][1:2, :] = squares

    return pl.pallas_call(
        body,
        grid=(width // block,),
        in_specs=[pl.BlockSpec((part, units), lambda n: (0, 0)) for _ in inputs]
        + [pl.BlockSpec((w.shape[0], block), lambda n: (0, n)) for w in weights],
        out_specs=[
            pl.BlockSpec((rows, block), lambda n: (0, n)),
            pl.BlockSpec((2, block), lambda n: (0, n)),
        ],
        out_shape=[
            jax.ShapeDtypeStruct((rows, width), float32),
            jax.ShapeDtypeStruct((2, width), float32),
        ],
        cost_estimate=pl.CostEstimate(
            flops=2 * rows * units * width,
            transcendentals=0,
            bytes_accessed=2 * rows * units + 2 * units * width + 4 * rows * width,
        ),
    )(*inputs, *weights)


def back_dot(slopes, weights, half):
    rows, width = slopes.shape
    middle = rows // 2

    def body(slope_ref, weight_ref, keep_ref, send_ref):
        product = dot_back(slope_ref[...], weight_ref[...])
        keep_ref[...] = product[:, :half]
        send_ref[:middle, :] = product[middle:, half:].astype(bfloat16)
        send_ref[middle:, :] = product[:middle, half:].astype(bfloat16)

    units = weights.shape[0] // 2
    return pl.pallas_call(
        body,
        grid=(units // half,),
        in_specs=[
            pl.BlockSpec(slopes.shape, lambda n: (0, 0)),
            pl.BlockSpec((2 * half, width), lambda n: (n, 0)),
        ],
        out_specs=[
            pl.BlockSpec((rows, half), lambda n: (0, n)),
            pl.BlockSpec((rows, half), lambda n: (0, n)),
        ],
        out_shape=[
            jax.ShapeDtypeStruct((rows, units), float32),
            jax.ShapeDtypeStruct((rows, units), bfloat16),
        ],
        cost_estimate=pl.CostEstimate(
            flops=4 * rows * width * units,
            transcendentals=0,
            bytes_accessed=2 * slopes.size + 2 * weights.size + 6 * rows * units,
        ),
    )(slopes, weights)


def weight_dot(inputs, slopes):
    part, units = inputs[0].shape
    width = slopes.shape[1]
    block = min(512, units)

    def body(*refs):
        slope_ref, out_ref = refs[-2:]
        product = 0.0
        for at, ref in enumerate(refs[:-2]):
            product = product + dot_rows(ref[...], slope_ref[at * part : (at + 1) * part, :])
        out_ref[...] = product.astype(bfloat16)

    return pl.pallas_call(
        body,
        grid=(units // block,),
        in_specs=[pl.BlockSpec((part, block), lambda n: (0, n)) for _ in inputs]
        + [pl.BlockSpec(slopes.shape, lambda n: (0, 0))],
        out_specs=pl.BlockSpec((block, width), lambda n: (n, 0)),
        out_shape=jax.ShapeDtypeStruct((units, width), bfloat16),
        cost_estimate=pl.CostEstimate(
            flops=2 * slopes.size * units,
            transcendentals=0,
            bytes_accessed=2 * slopes.shape[0] * units + 2 * slopes.size + 2 * units * width,
        ),
    )(*inputs, slopes)


def split_back_dot(slopes, top, end):
    rows, width = slopes.shape
    middle = rows // 2
    units = top.shape[0]
    block = min(512, units)
    steps = units // block

    def body(slope_ref, top_ref, end_ref, keep_ref, send_ref):
        def write(weight_ref):
            product = dot_back(slope_ref[...], weight_ref[...])
            keep_ref[...] = product[:middle]
            send_ref[...] = product[middle:].astype(bfloat16)

        at = pl.program_id(0)
        pl.when(at < steps)(lambda: write(top_ref))
        pl.when(at >= steps)(lambda: write(end_ref))

    return pl.pallas_call(
        body,
        grid=(2 * steps,),
        in_specs=[
            pl.BlockSpec(slopes.shape, lambda n: (0, 0)),
            pl.BlockSpec((block, width), lambda n: (jnp.minimum(n, steps - 1), 0)),
            pl.BlockSpec((block, width), lambda n: (jnp.maximum(n - steps, 0), 0)),
        ],
        out_specs=[
            pl.BlockSpec((middle, block), lambda n: (0, n)),
            pl.BlockSpec((middle, block), lambda n: (0, n)),
        ],
        out_shape=[
            jax.ShapeDtypeStruct((middle, 2 * units), float32),
            jax.ShapeDtypeStruct((middle, 2 * units), bfloat16),
        ],
        cost_estimate=pl.CostEstimate(
            flops=4 * rows * width * units,
            transcendentals=0,
            bytes_accessed=2 * slopes.size + 4 * units * width + 12 * middle * units,
        ),
    )(slopes, top, end)


def normalise(sums, axis, batch_total):
    totals, squares = total_of(sums, axis)
    average = totals / batch_total
    spread = squares / batch_total - average * average
    return average, 1.0 / jnp.sqrt(spread + epsilon_norm)


def flip_rows(array):
    half = array.shape[0] // 2
    return jnp.concatenate([array[half:], array[:half]])


def step(ids, hash_a, hash_b, hash_p, hash_m, w_in, w_mid, w_out, bn_gain, bn_bias, target):
    core = lax.axis_index("c")
    lane = lax.axis_index("x")
    first = core == 0
    mp = lax.axis_size("x")
    depth, height = lax.axis_size("z"), lax.axis_size("y")
    planes = depth * height
    rows, batch_devices = ids.shape[0], lax.axis_size(rows_axes)
    batch_total = rows * batch_devices
    width = w_in.shape[1]
    half = width // 2
    own = mp * half
    hidden = mp * width
    part = rows // mp
    out = w_out.shape[1]

    def in_order(mine, other):
        return jnp.where(first, mine, other), jnp.where(first, other, mine)

    def weight_part(layer, row, count):
        start = (layer, row, core * half)
        return lax.dynamic_slice(w_mid, start, (1, count, half)).reshape(count, half)

    w2_top = lax.all_gather(weight_part(0, 0, own), "x", axis=1, tiled=True)
    w2_near = weight_part(0, own, own)
    w2_far = [w2_near] + [
        lax.ppermute(w2_near, "x", [(i, i ^ k) for i in range(mp)]) for k in range(1, mp)
    ]
    w2_end = jnp.concatenate([lax.select_n(lane ^ k, *w2_far) for k in range(mp)], axis=1)
    w3_low, w3_high = jnp.split(weight_part(1, 0, hidden).reshape(mp, 2, half, half), 2, axis=1)
    w3_part = jnp.concatenate(in_order(w3_low, w3_high), axis=1).reshape(hidden, half)
    w3 = lax.all_gather(w3_part, "x", axis=1, tiled=True)

    def half_of(array, axis):
        return lax.dynamic_slice_in_dim(array, core * half, half, axis=axis)

    vectors = jnp.concatenate([half_of(bn_gain[1:], 1), half_of(bn_bias[1:], 1)])
    high = lax.reduce_precision(vectors, 8, 7)
    middle = lax.reduce_precision(vectors - high, 8, 7)
    low = vectors - high - middle
    small = jnp.concatenate(
        [
            half_of(w_out, 0).reshape(-1, width),
            jnp.concatenate([high, middle, low]).astype(bfloat16).reshape(-1, width),
        ]
    )
    small = jnp.pad(small, ((0, -small.shape[0] % 16), (0, 0)))
    target_own = lax.dynamic_slice_in_dim(target, lane * part, part, axis=0)
    wanted = jnp.concatenate([target_own, swap_cores(target_own)])

    encoded = encode(ids, hash_a, hash_b, hash_p, hash_m)
    z1 = dot(encoded, w_in)
    sums1 = (jnp.sum(z1, axis=0), jnp.sum(z1 * z1, axis=0))
    mean1, inv1 = normalise(sums1, over_rows, batch_total)
    n1 = (z1 - mean1) * inv1
    a1 = bn_gain[0] * n1 + bn_bias[0]
    x1 = mish_act(a1).astype(bfloat16)
    message = jnp.concatenate(
        [x1.reshape(mp, part, width), jnp.broadcast_to(small[None], (mp, *small.shape))], axis=1
    )
    message = lax.all_to_all(message, "x", 0, 0, tiled=True)
    x1_own = jnp.concatenate(list(message[:, :part]), axis=1)
    x1_other = swap_cores(x1_own)
    small = message[:, part:].reshape(mp, -1)
    w_out_own = small[:, : half * out].reshape(own, out)
    vectors = small[:, half * out : half * out + 12 * half].astype(float32)
    vectors = vectors.reshape(mp, 3, 4, half)
    vectors = vectors[:, 0] + vectors[:, 1] + vectors[:, 2]
    gain2, gain3, bias2, bias3 = vectors.transpose(1, 0, 2).reshape(4, own)
    z2, sums2 = layer_dot((x1_own, x1_other), (w2_top, w2_end))
    mean2, inv2 = normalise((sums2[0], sums2[1]), over_chips_x_last, batch_total)
    n2 = (z2 - mean2) * inv2
    a2 = gain2 * n2 + bias2
    x2 = mish_act(a2).astype(bfloat16)
    x2_other = swap_cores(flip_rows(x2))
    blocks = zip(jnp.split(x2, mp, axis=1), jnp.split(x2_other, mp, axis=1))
    x2_all = jnp.concatenate([block for pair in blocks for block in pair], axis=1)
    z3, sums3 = layer_dot((x2_all,), (w3,))
    mean3, inv3 = normalise((sums3[0], sums3[1]), over_chips, batch_total)
    n3 = (z3 - mean3) * inv3
    a3 = gain3 * n3 + bias3
    x3 = mish_act(a3).astype(bfloat16)

    y_part = dot(x3, w_out_own)
    predicted = y_part + swap_cores(flip_rows(y_part))
    g_y = ((predicted - wanted) / math.sqrt(batch_total)).astype(bfloat16)
    g_out = dot_rows(x3, g_y).reshape(mp, planes // 2, 2, -1, out)
    keep_out = jnp.where(first, g_out[:, :, 0], g_out[:, :, 1])
    send_out = jnp.where(first, g_out[:, :, 1], g_out[:, :, 0]).astype(bfloat16)
    keep_out = keep_out.astype(bfloat16)
    g_out = jnp.stack(in_order(keep_out, swap_cores(send_out)))
    g_out = g_out.transpose(0, 2, 1, 3, 4).reshape(depth, height * mp, -1)
    g_out = g_out.transpose(1, 0, 2).reshape(height * mp, 1, -1).astype(float32)

    u3 = dot_back(g_y, w_out_own)
    s3 = u3 * mish_slope(a3)
    bias_sum3, gain_sum3 = total_of((jnp.sum(s3, axis=0), jnp.sum(s3 * n3, axis=0)), over_chips)
    e3 = (gain3 * inv3 * (s3 - bias_sum3 / batch_total - n3 * gain_sum3 / batch_total)).astype(
        bfloat16
    )
    u2_keep, u2_send = back_dot(e3, w3, half)
    u2 = u2_keep + swap_cores(u2_send).astype(float32)
    dw3 = weight_dot((x2_all,), e3)
    dw3 = lax.psum_scatter(dw3, "z", scatter_dimension=0, tiled=True)
    dw3 = lax.psum_scatter(dw3, "x", scatter_dimension=1, tiled=True)

    s2 = u2 * mish_slope(a2)
    sums2 = jnp.concatenate([jnp.sum(s2, axis=0), jnp.sum(s2 * n2, axis=0)])
    count = sums2.shape[0]
    sums2 = jnp.broadcast_to(sums2[None, None], (height * mp, 1, count))
    sums2 = jnp.concatenate([sums2, g_out], axis=2)
    sums2 = jnp.sum(lax.all_to_all(sums2, ("y", "x"), 0, 0, tiled=True), axis=(0, 1))
    g_out = sums2[count:].reshape(depth, -1)
    sums2 = jnp.broadcast_to(sums2[None, :count], (depth, count))
    sums2 = jnp.concatenate([sums2, g_out], axis=1)[:, None]
    sums2 = jnp.sum(lax.all_to_all(sums2, "z", 0, 0, tiled=True), axis=(0, 1))
    bias_sum2, gain_sum2 = sums2[:own], sums2[own:count]
    grad_out = sums2[count:].reshape(-1, out)
    e2 = (gain2 * inv2 * (s2 - bias_sum2 / batch_total - n2 * gain_sum2 / batch_total)).astype(
        bfloat16
    )
    u1_keep, u1_send = split_back_dot(e2, w2_top, w2_end)
    u1_own = (u1_keep + swap_cores(u1_send).astype(float32)).astype(bfloat16)
    u1 = lax.all_to_all(u1_own, "x", 1, 0, tiled=True).astype(float32)
    dw2 = weight_dot((x1_own, x1_other), e2)
    dw2 = lax.psum_scatter(dw2, "z", scatter_dimension=0, tiled=True)
    dw2 = jnp.stack([b.reshape(height, -1, half) for b in jnp.split(dw2, mp, axis=1)], axis=1)
    dw2 = lax.all_to_all(dw2.reshape(height * mp, -1, half), ("y", "x"), 0, 0, tiled=True)
    dw2 = jnp.sum(dw2.astype(float32), axis=0)

    s1 = u1 * mish_slope(a1)
    bias_sum1, gain_sum1 = total_of((jnp.sum(s1, axis=0), jnp.sum(s1 * n1, axis=0)), over_rows)
    e1 = (
        bn_gain[0] * inv1 * (s1 - bias_sum1 / batch_total - n1 * gain_sum1 / batch_total)
    ).astype(bfloat16)
    dw1 = dot_rows(encoded, e1).reshape(planes, 2, -1, width)
    keep1 = jnp.where(first, dw1[:, 0], dw1[:, 1])
    send1 = jnp.where(first, dw1[:, 1], dw1[:, 0]).astype(bfloat16)
    dw1 = (keep1 + swap_cores(send1).astype(float32)).astype(bfloat16)
    dw1 = lax.all_to_all(dw1, plane, 0, 0, tiled=True)
    grad_first = jnp.sum(dw1.astype(float32), axis=0)

    dw2, dw3, grad_first = lax.optimization_barrier((dw2, dw3, grad_first))
    dw3 = dw3.reshape(2, half, half)
    dw3 = jnp.stack(in_order(dw3[0], dw3[1])).reshape(height, -1, half)
    dw3 = jnp.sum(lax.all_to_all(dw3, "y", 0, 0, tiled=True).astype(float32), axis=0)
    last = jnp.stack([dw2, dw3])
    low, high = jnp.split(last, 2, axis=1)
    other = swap_cores(jnp.where(first, high, low))
    grad_mid = jnp.concatenate(in_order(jnp.where(first, low, high), other), axis=2)

    sums = jnp.stack([gain_sum2, gain_sum3, bias_sum2, bias_sum3]).reshape(4, mp, half)
    mine = lax.dynamic_index_in_dim(sums, lane, axis=1, keepdims=False)
    later = jnp.concatenate(in_order(mine, swap_cores(mine)), axis=1)
    grad_gain = jnp.stack([gain_sum1, later[0], later[1]])
    grad_bias = jnp.stack([bias_sum1, later[2], later[3]])
    return (grad_first, grad_mid, grad_out, grad_gain, grad_bias)


def solution(mesh):
    grid = Mesh(mesh.devices.reshape(4, 4, 2, 4), ("z", "y", "c", "x"))
    return jax.shard_map(
        step,
        mesh=grid,
        in_specs=(
            P(rows_axes),
            P(),
            P(),
            P(),
            P(),
            P(None, "x"),
            P(None, None, "x"),
            P("x", None),
            P(None, "x"),
            P(None, "x"),
            P(rows_axes, None),
        ),
        out_specs=(
            P(rows_axes, "x"),
            P(None, rows_axes, "x"),
            P(("x", "z", "y", "c"), None),
            P(None, "x"),
            P(None, "x"),
        ),
        check_vma=False,
    )
```

```python
import math

import jax
import jax.numpy as jnp
from jax import lax
from jax.experimental import pallas as pl
from jax.sharding import Mesh, PartitionSpec as P

epsilon_norm = 1e-05
plane = ("z", "y")
over_chips = (("z", "y", "x"),)
over_chips_x_last = (("z", "y"), "x")
over_rows = ("c", ("z", "y"))
rows_axes = ("z", "y", "c")
float32 = jnp.float32
bfloat16 = jnp.bfloat16


def swap_cores(array):
    return lax.ppermute(array, "c", [(0, 1), (1, 0)])


def from_everyone(array, axis):
    size = lax.axis_size(axis)
    return lax.all_to_all(
        jnp.broadcast_to(array[None], (size, *array.shape)), axis, 0, 0, tiled=True
    )


def sum_over(rows, stages):
    for axis in stages:
        if axis == "c":
            rows = rows + swap_cores(rows)
        else:
            rows = jnp.sum(from_everyone(rows, axis), axis=0)
    return rows[0]


def total_of(pair, stages):
    return jnp.split(sum_over(jnp.concatenate(pair)[None], stages), len(pair))


def float_mod(values, inverse, modulus):
    rest = values - jnp.floor(values * inverse) * modulus
    return jnp.where(rest >= modulus, rest - modulus, rest)


def encode(ids, hash_a, hash_b, hash_p, hash_m):
    modulus = hash_p.astype(float32)[None, :]
    buckets = hash_m.astype(float32)[None, :]
    below = 1.0 - 2.0**-21
    inverse_p = below / modulus
    inverse_m = below / buckets
    high = (hash_a // 128).astype(float32)[None, :]
    low = (hash_a % 128).astype(float32)[None, :]
    shift = hash_b.astype(float32)[None, :]
    step = 2.0 / (buckets - 1.0)
    reduced = float_mod(ids.astype(float32)[:, None], inverse_p, modulus)
    carried = float_mod(high * reduced, inverse_p, modulus)
    mixed = float_mod(carried * 128.0 + low * reduced + shift, inverse_p, modulus)
    hashed = float_mod(mixed, inverse_m, buckets)
    return lax.optimization_barrier((hashed * step - 1.0).astype(bfloat16))


def mish_act(values):
    power = jnp.exp(jnp.minimum(values, 30.0))
    ratio = power * (power + 2.0)
    return values * (ratio / (ratio + 2.0))


def mish_slope(values):
    power = jnp.exp(jnp.minimum(values, 30.0))
    ratio = power * (power + 2.0)
    inverse = 1.0 / (ratio + 2.0)
    return inverse * (ratio + 4.0 * values * (power * (power + 1.0)) * inverse)


def dot(left, right):
    return jnp.dot(left, right, preferred_element_type=float32)


def dot_rows(left, right):
    return lax.dot_general(left, right, (((0,), (0,)), ((), ())), preferred_element_type=float32)


def dot_back(left, right):
    return lax.dot_general(left, right, (((1,), (1,)), ((), ())), preferred_element_type=float32)


def layer_dot(inputs, weights):
    part, units = inputs[0].shape
    rows, width = part * len(inputs), weights[0].shape[1]
    block = min(256, width)

    def body(*refs):
        input_refs, weight_refs = refs[: len(inputs)], refs[len(inputs) : -2]
        totals, squares = 0.0, 0.0
        for at, input_ref in enumerate(input_refs):
            product = 0.0
            start = 0
            for ref in weight_refs:
                end = start + ref.shape[0]
                product = product + dot(input_ref[:, start:end], ref[...])
                start = end
            refs[-2][at * part : (at + 1) * part, :] = product
            totals = totals + jnp.sum(product, axis=0, keepdims=True)
            squares = squares + jnp.sum(product * product, axis=0, keepdims=True)
        refs[-1][0:1, :] = totals
        refs[-1][1:2, :] = squares

    return pl.pallas_call(
        body,
        grid=(width // block,),
        in_specs=[pl.BlockSpec((part, units), lambda n: (0, 0)) for _ in inputs]
        + [pl.BlockSpec((w.shape[0], block), lambda n: (0, n)) for w in weights],
        out_specs=[
            pl.BlockSpec((rows, block), lambda n: (0, n)),
            pl.BlockSpec((2, block), lambda n: (0, n)),
        ],
        out_shape=[
            jax.ShapeDtypeStruct((rows, width), float32),
            jax.ShapeDtypeStruct((2, width), float32),
        ],
        cost_estimate=pl.CostEstimate(
            flops=2 * rows * units * width,
            transcendentals=0,
            bytes_accessed=2 * rows * units + 2 * units * width + 4 * rows * width,
        ),
    )(*inputs, *weights)


def back_dot(slopes, weights, half, offset, dtype, flip):
    rows, width = slopes.shape
    middle = rows // 2
    units = weights.shape[0] // 2

    def body(slope_ref, weight_ref, out_ref):
        product = dot_back(slope_ref[...], weight_ref[...]).astype(dtype)
        if flip:
            out_ref[:middle, :] = product[middle:]
            out_ref[middle:, :] = product[:middle]
        else:
            out_ref[...] = product

    return pl.pallas_call(
        body,
        grid=(units // half,),
        in_specs=[
            pl.BlockSpec(slopes.shape, lambda n: (0, 0)),
            pl.BlockSpec((half, width), lambda n: (2 * n + offset, 0)),
        ],
        out_specs=pl.BlockSpec((rows, half), lambda n: (0, n)),
        out_shape=jax.ShapeDtypeStruct((rows, units), dtype),
        cost_estimate=pl.CostEstimate(
            flops=2 * rows * width * units,
            transcendentals=0,
            bytes_accessed=2 * slopes.size + weights.size + 3 * rows * units,
        ),
    )(slopes, weights)


def weight_dot(inputs, slopes):
    part, units = inputs[0].shape
    width = slopes.shape[1]
    block = min(512, units)

    def body(*refs):
        slope_ref, out_ref = refs[-2:]
        product = 0.0
        for at, ref in enumerate(refs[:-2]):
            product = product + dot_rows(ref[...], slope_ref[at * part : (at + 1) * part, :])
        out_ref[...] = product.astype(bfloat16)

    return pl.pallas_call(
        body,
        grid=(units // block,),
        in_specs=[pl.BlockSpec((part, block), lambda n: (0, n)) for _ in inputs]
        + [pl.BlockSpec(slopes.shape, lambda n: (0, 0))],
        out_specs=pl.BlockSpec((block, width), lambda n: (n, 0)),
        out_shape=jax.ShapeDtypeStruct((units, width), bfloat16),
        cost_estimate=pl.CostEstimate(
            flops=2 * slopes.size * units,
            transcendentals=0,
            bytes_accessed=2 * slopes.shape[0] * units + 2 * slopes.size + 2 * units * width,
        ),
    )(*inputs, slopes)


def split_back_dot(slopes, top, end, part_at, dtype):
    rows, width = slopes.shape
    middle = rows // 2
    units = top.shape[0]
    block = min(512, units)
    steps = units // block

    def body(slope_ref, top_ref, end_ref, out_ref):
        def write(weight_ref):
            out_ref[...] = dot_back(slope_ref[...], weight_ref[...]).astype(dtype)

        at = pl.program_id(0)
        pl.when(at < steps)(lambda: write(top_ref))
        pl.when(at >= steps)(lambda: write(end_ref))

    return pl.pallas_call(
        body,
        grid=(2 * steps,),
        in_specs=[
            pl.BlockSpec((middle, width), lambda n: (part_at, 0)),
            pl.BlockSpec((block, width), lambda n: (jnp.minimum(n, steps - 1), 0)),
            pl.BlockSpec((block, width), lambda n: (jnp.maximum(n - steps, 0), 0)),
        ],
        out_specs=pl.BlockSpec((middle, block), lambda n: (0, n)),
        out_shape=jax.ShapeDtypeStruct((middle, 2 * units), dtype),
        cost_estimate=pl.CostEstimate(
            flops=4 * middle * width * units,
            transcendentals=0,
            bytes_accessed=slopes.size + 4 * units * width + 6 * middle * units,
        ),
    )(slopes, top, end)


def normalise(sums, axis, batch_total):
    totals, squares = total_of(sums, axis)
    average = totals / batch_total
    spread = squares / batch_total - average * average
    return average, 1.0 / jnp.sqrt(spread + epsilon_norm)


def flip_rows(array):
    half = array.shape[0] // 2
    return jnp.concatenate([array[half:], array[:half]])


def step(ids, hash_a, hash_b, hash_p, hash_m, w_in, w_mid, w_out, bn_gain, bn_bias, target):
    core = lax.axis_index("c")
    lane = lax.axis_index("x")
    first = core == 0
    mp = lax.axis_size("x")
    depth, height = lax.axis_size("z"), lax.axis_size("y")
    planes = depth * height
    rows, batch_devices = ids.shape[0], lax.axis_size(rows_axes)
    batch_total = rows * batch_devices
    width = w_in.shape[1]
    half = width // 2
    own = mp * half
    hidden = mp * width
    part = rows // mp
    out = w_out.shape[1]

    def in_order(mine, other):
        return jnp.where(first, mine, other), jnp.where(first, other, mine)

    def weight_part(layer, row, count):
        start = (layer, row, core * half)
        return lax.dynamic_slice(w_mid, start, (1, count, half)).reshape(count, half)

    w2_top = lax.all_gather(weight_part(0, 0, own), "x", axis=1, tiled=True)
    w2_near = weight_part(0, own, own)
    w2_far = [w2_near] + [
        lax.ppermute(w2_near, "x", [(i, i ^ k) for i in range(mp)]) for k in range(1, mp)
    ]
    w2_end = jnp.concatenate([lax.select_n(lane ^ k, *w2_far) for k in range(mp)], axis=1)
    w3_low, w3_high = jnp.split(weight_part(1, 0, hidden).reshape(mp, 2, half, half), 2, axis=1)
    w3_part = jnp.concatenate(in_order(w3_low, w3_high), axis=1).reshape(hidden, half)
    w3 = lax.all_gather(w3_part, "x", axis=1, tiled=True)

    def half_of(array, axis):
        return lax.dynamic_slice_in_dim(array, core * half, half, axis=axis)

    vectors = jnp.concatenate([half_of(bn_gain[1:], 1), half_of(bn_bias[1:], 1)])
    high = lax.reduce_precision(vectors, 8, 7)
    middle = lax.reduce_precision(vectors - high, 8, 7)
    low = vectors - high - middle
    small = jnp.concatenate(
        [
            half_of(w_out, 0).reshape(-1, width),
            jnp.concatenate([high, middle, low]).astype(bfloat16).reshape(-1, width),
        ]
    )
    small = jnp.pad(small, ((0, -small.shape[0] % 16), (0, 0)))
    target_own = lax.dynamic_slice_in_dim(target, lane * part, part, axis=0)
    wanted = jnp.concatenate([target_own, swap_cores(target_own)])

    encoded = encode(ids, hash_a, hash_b, hash_p, hash_m)
    z1 = dot(encoded, w_in)
    sums1 = (jnp.sum(z1, axis=0), jnp.sum(z1 * z1, axis=0))
    mean1, inv1 = normalise(sums1, over_rows, batch_total)
    n1 = (z1 - mean1) * inv1
    a1 = bn_gain[0] * n1 + bn_bias[0]
    x1 = mish_act(a1).astype(bfloat16)
    message = jnp.concatenate(
        [x1.reshape(mp, part, width), jnp.broadcast_to(small[None], (mp, *small.shape))], axis=1
    )
    message = lax.all_to_all(message, "x", 0, 0, tiled=True)
    x1_own = jnp.concatenate(list(message[:, :part]), axis=1)
    x1_other = swap_cores(x1_own)
    small = message[:, part:].reshape(mp, -1)
    w_out_own = small[:, : half * out].reshape(own, out)
    vectors = small[:, half * out : half * out + 12 * half].astype(float32)
    vectors = vectors.reshape(mp, 3, 4, half)
    vectors = vectors[:, 0] + vectors[:, 1] + vectors[:, 2]
    gain2, gain3, bias2, bias3 = vectors.transpose(1, 0, 2).reshape(4, own)
    z2, sums2 = layer_dot((x1_own, x1_other), (w2_top, w2_end))
    mean2, inv2 = normalise((sums2[0], sums2[1]), over_chips_x_last, batch_total)
    n2 = (z2 - mean2) * inv2
    a2 = gain2 * n2 + bias2
    x2 = mish_act(a2).astype(bfloat16)
    x2_other = swap_cores(flip_rows(x2))
    blocks = zip(jnp.split(x2, mp, axis=1), jnp.split(x2_other, mp, axis=1))
    x2_all = jnp.concatenate([block for pair in blocks for block in pair], axis=1)
    z3, sums3 = layer_dot((x2_all,), (w3,))
    mean3, inv3 = normalise((sums3[0], sums3[1]), over_chips, batch_total)
    n3 = (z3 - mean3) * inv3
    a3 = gain3 * n3 + bias3
    x3 = mish_act(a3).astype(bfloat16)

    y_part = dot(x3, w_out_own)
    predicted = y_part + swap_cores(flip_rows(y_part))
    g_y = ((predicted - wanted) / math.sqrt(batch_total)).astype(bfloat16)
    g_out = dot_rows(x3, g_y).reshape(mp, planes // 2, 2, -1, out)
    keep_out = jnp.where(first, g_out[:, :, 0], g_out[:, :, 1])
    send_out = jnp.where(first, g_out[:, :, 1], g_out[:, :, 0]).astype(bfloat16)
    keep_out = keep_out.astype(bfloat16)
    g_out = jnp.stack(in_order(keep_out, swap_cores(send_out)))
    g_out = g_out.transpose(0, 2, 1, 3, 4).reshape(depth, height * mp, -1)
    g_out = g_out.transpose(1, 0, 2).reshape(height * mp, 1, -1).astype(float32)

    u3 = dot_back(g_y, w_out_own)
    s3 = u3 * mish_slope(a3)
    bias_sum3, gain_sum3 = total_of((jnp.sum(s3, axis=0), jnp.sum(s3 * n3, axis=0)), over_chips)
    e3 = (gain3 * inv3 * (s3 - bias_sum3 / batch_total - n3 * gain_sum3 / batch_total)).astype(
        bfloat16
    )
    u2_far = swap_cores(back_dot(e3, w3, half, 1, bfloat16, True))
    u2 = back_dot(e3, w3, half, 0, float32, False) + u2_far.astype(float32)
    dw3 = weight_dot((x2_all,), e3)
    dw3 = lax.psum_scatter(dw3, "z", scatter_dimension=0, tiled=True)
    dw3 = lax.psum_scatter(dw3, "x", scatter_dimension=1, tiled=True)

    s2 = u2 * mish_slope(a2)
    sums2 = jnp.concatenate([jnp.sum(s2, axis=0), jnp.sum(s2 * n2, axis=0)])
    count = sums2.shape[0]
    sums2 = jnp.broadcast_to(sums2[None, None], (height * mp, 1, count))
    sums2 = jnp.concatenate([sums2, g_out], axis=2)
    sums2 = jnp.sum(lax.all_to_all(sums2, ("y", "x"), 0, 0, tiled=True), axis=(0, 1))
    g_out = sums2[count:].reshape(depth, -1)
    sums2 = jnp.broadcast_to(sums2[None, :count], (depth, count))
    sums2 = jnp.concatenate([sums2, g_out], axis=1)[:, None]
    sums2 = jnp.sum(lax.all_to_all(sums2, "z", 0, 0, tiled=True), axis=(0, 1))
    bias_sum2, gain_sum2 = sums2[:own], sums2[own:count]
    grad_out = sums2[count:].reshape(-1, out)
    e2 = (gain2 * inv2 * (s2 - bias_sum2 / batch_total - n2 * gain_sum2 / batch_total)).astype(
        bfloat16
    )
    u1_far = swap_cores(split_back_dot(e2, w2_top, w2_end, 1, bfloat16))
    u1_own = split_back_dot(e2, w2_top, w2_end, 0, float32) + u1_far.astype(float32)
    u1_own = u1_own.astype(bfloat16)
    u1 = lax.all_to_all(u1_own, "x", 1, 0, tiled=True).astype(float32)
    dw2 = weight_dot((x1_own, x1_other), e2)
    dw2 = lax.psum_scatter(dw2, "z", scatter_dimension=0, tiled=True)
    dw2 = jnp.stack([b.reshape(height, -1, half) for b in jnp.split(dw2, mp, axis=1)], axis=1)
    dw2 = lax.all_to_all(dw2.reshape(height * mp, -1, half), ("y", "x"), 0, 0, tiled=True)
    dw2 = jnp.sum(dw2.astype(float32), axis=0)

    s1 = u1 * mish_slope(a1)
    bias_sum1, gain_sum1 = total_of((jnp.sum(s1, axis=0), jnp.sum(s1 * n1, axis=0)), over_rows)
    e1 = (
        bn_gain[0] * inv1 * (s1 - bias_sum1 / batch_total - n1 * gain_sum1 / batch_total)
    ).astype(bfloat16)
    dw1 = dot_rows(encoded, e1).reshape(planes, 2, -1, width)
    keep1 = jnp.where(first, dw1[:, 0], dw1[:, 1])
    send1 = jnp.where(first, dw1[:, 1], dw1[:, 0]).astype(bfloat16)
    dw1 = (keep1 + swap_cores(send1).astype(float32)).astype(bfloat16)
    dw1 = lax.all_to_all(dw1, plane, 0, 0, tiled=True)
    grad_first = jnp.sum(dw1.astype(float32), axis=0)

    dw2, dw3, grad_first = lax.optimization_barrier((dw2, dw3, grad_first))
    dw3 = dw3.reshape(2, half, half)
    dw3 = jnp.stack(in_order(dw3[0], dw3[1])).reshape(height, -1, half)
    dw3 = jnp.sum(lax.all_to_all(dw3, "y", 0, 0, tiled=True).astype(float32), axis=0)
    last = jnp.stack([dw2, dw3])
    low, high = jnp.split(last, 2, axis=1)
    other = swap_cores(jnp.where(first, high, low))
    grad_mid = jnp.concatenate(in_order(jnp.where(first, low, high), other), axis=2)

    sums = jnp.stack([gain_sum2, gain_sum3, bias_sum2, bias_sum3]).reshape(4, mp, half)
    mine = lax.dynamic_index_in_dim(sums, lane, axis=1, keepdims=False)
    later = jnp.concatenate(in_order(mine, swap_cores(mine)), axis=1)
    grad_gain = jnp.stack([gain_sum1, later[0], later[1]])
    grad_bias = jnp.stack([bias_sum1, later[2], later[3]])
    return (grad_first, grad_mid, grad_out, grad_gain, grad_bias)


def solution(mesh):
    grid = Mesh(mesh.devices.reshape(4, 4, 2, 4), ("z", "y", "c", "x"))
    return jax.shard_map(
        step,
        mesh=grid,
        in_specs=(
            P(rows_axes),
            P(),
            P(),
            P(),
            P(),
            P(None, "x"),
            P(None, None, "x"),
            P("x", None),
            P(None, "x"),
            P(None, "x"),
            P(rows_axes, None),
        ),
        out_specs=(
            P(rows_axes, "x"),
            P(None, rows_axes, "x"),
            P(("x", "z", "y", "c"), None),
            P(None, "x"),
            P(None, "x"),
        ),
        check_vma=False,
    )
```
